8 devices in a mesh: rep: 1 (over z), data: 2 (over y), expert: 4 (over x, core).
Axes of the slice: x: 2, y: 2, z: 1, core: 2. Of those that a mesh axis runs over, the one named last changes fastest.
Arguments:
- x_in: bfloat16 [2, 16384, 768], P(None, ('rep', 'expert', 'data'))
- expert_idx: int32 [2, 16384, 1], P(None, ('rep', 'expert', 'data'))
- gate_wt: float32 [2, 16384, 1], P(None, ('rep', 'expert', 'data'))
- w_gate: bfloat16 [8, 768, 3072], P('expert', 'data')
- w_up: bfloat16 [8, 768, 3072], P('expert', 'data')
- w_down: bfloat16 [8, 3072, 768], P('expert', None, 'data')
Outputs:
- output: bfloat16 [2, 16384, 768], P(None, ('rep', 'expert', 'data'))
All inputs are finite; a program needn't handle non-finite values.
Results may differ from the reference program's by a relative error of at most 0.001.
Values are sent between devices in bfloat16 or wider.
A program may use at most 1 GiB of HBM per device.

```python
import jax
import jax.numpy as jnp
from jax import lax

D_MODEL = 768
FF = 3072
N_EXP = 8
TOP = 1
TOK_LOC = 2048
EXPERT_DEVS = 4
DATA_DEVS = 2
CAP = 320


def draw_routing(route_key):
    dev_count = EXPERT_DEVS * DATA_DEVS
    key_noise, key_bias, key_hot, key_perm = jax.random.split(route_key, 4)
    draw_noise = jax.random.randint(key_noise, (2, dev_count, TOK_LOC, N_EXP), 0, 4096)
    exp_bias = jax.random.randint(key_bias, (2, 1, 1, N_EXP), 0, 1024)
    hot_id = jax.random.randint(key_hot, (2, dev_count, 1, 1), 0, N_EXP)
    perm_keys = jax.random.split(key_perm, 2 * dev_count)
    tok_rank = jax.vmap(lambda sub_key: jax.random.permutation(sub_key, TOK_LOC))(perm_keys)
    tok_rank = tok_rank.reshape(2, dev_count, TOK_LOC, 1)
    hot_count = min(TOK_LOC, CAP + CAP // 4)
    expert_ids = jnp.arange(N_EXP, dtype=jnp.int32)
    forced = jnp.logical_and(tok_rank < hot_count, expert_ids == hot_id).astype(jnp.int32)
    int_score = (draw_noise + exp_bias + forced * 8192) * N_EXP + expert_ids
    chosen = lax.top_k(int_score, TOP)[1].astype(jnp.int32)
    return chosen.reshape(2, dev_count * TOK_LOC, TOP)


def setup_inputs(seed: int = 0, part: int = 0) -> dict:
    base_key = jax.random.key(seed)
    shared_key, token_key = jax.random.split(base_key)
    part_key = jax.random.fold_in(token_key, part)
    key_x, key_route, key_gate = jax.random.split(part_key, 3)
    key_wg, key_wu, key_wd = jax.random.split(shared_key, 3)
    tok_all = EXPERT_DEVS * DATA_DEVS * TOK_LOC
    x_in = jax.random.normal(key_x, (2, tok_all, D_MODEL), jnp.float32).astype(jnp.bfloat16)
    expert_idx = draw_routing(key_route)
    gate_wt = jax.random.uniform(key_gate, (2, tok_all, TOP), jnp.float32, 0.2, 0.8)
    w_gate = (jax.random.normal(key_wg, (N_EXP, D_MODEL, FF), jnp.float32) * D_MODEL ** -0.5).astype(jnp.bfloat16)
    w_up = (jax.random.normal(key_wu, (N_EXP, D_MODEL, FF), jnp.float32) * D_MODEL ** -0.5).astype(jnp.bfloat16)
    w_down = (jax.random.normal(key_wd, (N_EXP, FF, D_MODEL), jnp.float32) * (1.5 * FF ** -0.5)).astype(jnp.bfloat16)
    return {'x_in': x_in, 'expert_idx': expert_idx, 'gate_wt': gate_wt, 'w_gate': w_gate, 'w_up': w_up, 'w_down': w_down}


def slot_table(ids_block):
    flat_ids = ids_block.reshape(-1)
    one_hot = (flat_ids[:, None] == jnp.arange(N_EXP, dtype=jnp.int32)[None, :]).astype(jnp.int32)
    slot_of = jnp.sum((jnp.cumsum(one_hot, axis=0) - one_hot) * one_hot, axis=1)
    return flat_ids, slot_of


def expert_ffn(rows_in, wg_one, wu_one, wd_one):
    gate_pre = jnp.dot(rows_in, wg_one, preferred_element_type=jnp.float32)
    up_pre = jnp.dot(rows_in, wu_one, preferred_element_type=jnp.float32)
    hidden = (jax.nn.silu(gate_pre) * up_pre).astype(jnp.bfloat16)
    return jnp.dot(hidden, wd_one, preferred_element_type=jnp.float32).astype(jnp.bfloat16)


def moe_micro(x_mb, idx_mb, gate_mb, w_gate, w_up, w_down):
    dev_count = EXPERT_DEVS * DATA_DEVS
    pair_count = TOK_LOC * TOP
    slot_total = N_EXP * CAP
    x_blocks = x_mb.reshape(dev_count, TOK_LOC, D_MODEL)
    flat_ids, slot_of = jax.vmap(slot_table)(idx_mb.reshape(dev_count, TOK_LOC, TOP))
    is_kept = slot_of < CAP
    dest_pos = jnp.where(is_kept, flat_ids * CAP + slot_of, slot_total)
    pair_ids = jnp.arange(pair_count, dtype=jnp.int32)
    source_of = jax.vmap(lambda dest_row: jnp.full((slot_total,), pair_count, jnp.int32).at[dest_row].set(pair_ids, mode='drop'))(dest_pos)
    tok_of = jnp.minimum(source_of // TOP, TOK_LOC - 1)
    buffers = jax.vmap(lambda x_blk, tok_row: x_blk[tok_row])(x_blocks, tok_of)
    buffers = jnp.where((source_of < pair_count)[:, :, None], buffers, jnp.zeros((), jnp.bfloat16))
    per_expert = buffers.reshape(dev_count, N_EXP, CAP, D_MODEL).transpose(1, 0, 2, 3).reshape(N_EXP, dev_count * CAP, D_MODEL)
    expert_out = lax.map(lambda expert_args: expert_ffn(expert_args[0], expert_args[1], expert_args[2], expert_args[3]), (per_expert, w_gate, w_up, w_down))
    back_rows = expert_out.reshape(N_EXP, dev_count, CAP, D_MODEL).transpose(1, 0, 2, 3).reshape(dev_count, slot_total, D_MODEL)
    pair_out = jax.vmap(lambda back_blk, pos_row: back_blk[pos_row])(back_rows, jnp.minimum(dest_pos, slot_total - 1))
    pair_out = pair_out.reshape(dev_count, TOK_LOC, TOP, D_MODEL).astype(jnp.float32)
    weight = jnp.where(is_kept.reshape(dev_count, TOK_LOC, TOP), gate_mb.reshape(dev_count, TOK_LOC, TOP), 0.0)
    mix_sum = jnp.sum(pair_out * weight[:, :, :, None], axis=2)
    y_blocks = (x_blocks.astype(jnp.float32) + mix_sum).astype(jnp.bfloat16)
    return y_blocks.reshape(dev_count * TOK_LOC, D_MODEL)


def reference(x_in, expert_idx, gate_wt, w_gate, w_up, w_down):
    return lax.map(lambda mb_args: moe_micro(mb_args[0], mb_args[1], mb_args[2], w_gate, w_up, w_down), (x_in, expert_idx, gate_wt))
```

```python
import functools

import jax
import jax.numpy as jnp
from jax import lax
from jax.experimental import pallas as pl
from jax.experimental.pallas import tpu as pltpu
from jax.sharding import PartitionSpec as P

F32 = jnp.float32
BF16 = jnp.bfloat16
LANES = 128


def dot(a, b):
    return jnp.dot(a, b, preferred_element_type=F32)


def moe_kernel(dims, ids_ref, gate_ref, x_hbm, wg_hbm, wu_hbm, wd_hbm, y_hbm,
               xbuf, send, recv, back, oacc, wg_buf, wu_buf, wd_buf, p_buf, c_buf, slot_buf, cat_buf, col_buf,
               x_sem, y_sem, tok_send, tok_recv, ret_send, ret_recv, w_send, w_recv, w_loc, credit, go):
    cap, fc, nf = dims
    n_mb, tok, d_model = xbuf.shape
    half = d_model // 2
    groups = tok // LANES
    q_me = lax.axis_index('expert')
    y_me = lax.axis_index('data')
    x_me, c_me = lax.div(q_me, 2), lax.rem(q_me, 2)

    def piece(i):
        j = lax.div(i, 8)
        mb = lax.rem(lax.div(i, 4), 2)
        o = lax.rem(i, 4)
        hi = 1 - lax.div(o, 2)
        pp = lax.rem(o, 2)
        return j, mb, o, hi, pp

    def partner(hi, pp):
        return {'expert': lax.rem(x_me + hi, 2) * 2 + lax.rem(c_me + pp, 2)}

    def tok_copy(i):
        j, mb, o, hi, pp = piece(i)
        dst = recv.at[j, (1 - hi) * 2 + mb, pl.ds(pp * cap, cap), :]
        return pltpu.make_async_remote_copy(send.at[i], dst, tok_send.at[i], tok_recv.at[i], device_id=partner(hi, pp))

    def ret_copy(i):
        j, mb, o, hi, pp = piece(i)
        src = recv.at[j, (1 - hi) * 2 + mb, pl.ds(pp * cap, cap), :]
        dst = back.at[j, mb, pp, pl.ds(hi * cap, cap), :]
        return pltpu.make_async_remote_copy(src, dst, ret_send.at[i], ret_recv.at[i], device_id=partner(hi, pp))

    y_other = {'data': 1 - y_me}
    my_half = pl.ds(pl.multiple_of(y_me * half, half), half)

    def w_parts(j, k):
        cols = pl.ds(pl.multiple_of(k * fc, fc), fc)
        return ((wg_hbm.at[j, :, cols], wg_buf.at[k, my_half, :], 0),
                (wu_hbm.at[j, :, cols], wu_buf.at[k, my_half, :], 1),
                (wd_hbm.at[j, cols, :], wd_buf.at[k, :, my_half], 2))

    def w_remote(j, k):
        return [pltpu.make_async_remote_copy(s, d, w_send.at[k, n], w_recv.at[k, n], device_id=y_other)
                for s, d, n in w_parts(j, k)]

    def w_local(j, k):
        return [pltpu.make_async_copy(s, d, w_loc.at[k, n]) for s, d, n in w_parts(j, k)]

    barrier = pltpu.get_barrier_semaphore()
    for dev in (partner(0, 1), partner(1, 0), partner(1, 1), y_other):
        pl.semaphore_signal(barrier, inc=1, device_id=dev)
    pl.semaphore_wait(barrier, 4)

    def start_first(k, _):
        for c in w_remote(0, k):
            c.start()
        return 0

    @pl.when(c_me == 0)
    def _():
        lax.fori_loop(0, nf, start_first, 0)

    x_loads = [pltpu.make_async_copy(x_hbm.at[mb], xbuf.at[mb], x_sem.at[mb]) for mb in range(n_mb)]
    for c in x_loads:
        c.start()

    def start_local(k, _):
        for c in w_local(0, k):
            c.start()
        return 0

    lax.fori_loop(0, nf, start_local, 0)

    masks = []
    for mb in range(n_mb):
        ids = ids_ref[mb]
        for e in range(8):
            masks.append((ids == e).astype(F32))
    stack = jnp.concatenate(masks, axis=0).astype(BF16)
    rows = stack.shape[0]
    lane_r = lax.broadcasted_iota(jnp.int32, (LANES, LANES), 0)
    lane_c = lax.broadcasted_iota(jnp.int32, (LANES, LANES), 1)
    upper = jnp.where(lane_r < lane_c, 1.0, 0.0).astype(BF16)
    row_r = lax.broadcasted_iota(jnp.int32, (rows, rows), 0)
    row_c = lax.broadcasted_iota(jnp.int32, (rows, rows), 1)
    first = row_r - lax.rem(row_r, groups)
    lower = jnp.where((row_c >= first) & (row_c < row_r), 1.0, 0.0).astype(BF16)
    ones = jnp.ones((LANES, LANES), BF16)
    prefix = dot(stack, upper) + dot(dot(lower, stack).astype(BF16), ones)
    cat_buf[...] = jnp.zeros_like(cat_buf)
    for mb in range(n_mb):
        place = jnp.full((groups, LANES), -1.0, F32)
        for e in range(8):
            r0 = (mb * 8 + e) * groups
            slot = prefix[r0:r0 + groups]
            j, qe = e % 2, e // 2
            hi = lax.rem(x_me + qe // 2, 2)
            pp = lax.rem(c_me + qe % 2, 2)
            base = (((j * 2 + pp) * 2 + hi) * cap).astype(F32)
            place = jnp.where((masks[mb * 8 + e] > 0.5) & (slot < float(cap)), base + slot, place)
        slot_buf[mb] = place
        cat_buf[mb, 0:groups, :] = place
        cat_buf[mb, groups:2 * groups, :] = gate_ref[mb]
        col_buf[mb] = cat_buf[mb].T

    for c in x_loads:
        c.wait()

    def dispatch(i, _):
        j, mb, o, hi, pp = piece(i)
        base = (((j * 2 + pp) * 2 + hi) * cap).astype(F32)
        want = lax.broadcasted_iota(jnp.int32, (cap, LANES), 0).astype(F32) + base
        place = slot_buf[mb]
        for g in range(groups):
            p_buf[:, g * LANES:(g + 1) * LANES] = jnp.where(place[g:g + 1, :] == want, 1.0, 0.0).astype(BF16)
        out = dot(p_buf[...], xbuf[mb]).astype(BF16)

        @pl.when(o == 2)
        def _():
            recv[j, 2 + mb, 0:cap, :] = out

        @pl.when(o != 2)
        def _():
            send[i] = out

        @pl.when((i > 0) & (o != 3))
        def _():
            tok_copy(i - 1).start()

        return 0

    lax.fori_loop(0, 16, dispatch, 0)
    tok_copy(15).start()

    @pl.when(c_me == 1)
    def _():
        pl.semaphore_wait(go, 1)
        lax.fori_loop(0, nf, start_first, 0)

    def wait_tokens(j):
        for r in range(8):
            if r % 4 != 2:
                tok_copy(j * 8 + r).wait_recv()

    def wait_weights(j, k):
        for c in w_local(j, k):
            c.wait()
        for c in w_remote(j, k):
            c.wait()

    def hidden_times_down(rows_in, k):
        gate_pre = dot(rows_in, wg_buf[k])
        up_pre = dot(rows_in, wu_buf[k])
        hidden = (gate_pre / (1.0 + jnp.exp(-gate_pre)) * up_pre).astype(BF16)
        return dot(hidden, wd_buf[k])

    def expert(j):
        oacc[...] = jnp.zeros_like(oacc)
        wait_tokens(j)

        def chunk(k, _):
            wait_weights(j, k)

            def block(b, _):
                oacc[b] += hidden_times_down(recv[j, b], k)
                return 0

            lax.fori_loop(0, 4, block, 0)
            if j == 0:
                pl.semaphore_signal(credit, inc=1, device_id=y_other)
                pl.semaphore_wait(credit, 1)
                for c in w_remote(1, k) + w_local(1, k):
                    c.start()
            else:
                @pl.when((k == nf - 3) & (c_me == 0))
                def _():
                    pl.semaphore_signal(go, inc=1, device_id=partner(0, 1))
            return 0

        lax.fori_loop(0, nf - 1, chunk, 0)
        last = nf - 1
        wait_weights(j, last)

        def index_of(r):
            b, pp = lax.div(r, 2), lax.rem(r, 2)
            return j * 8 + lax.rem(b, 2) * 4 + lax.div(b, 2) * 2 + pp

        def finish(r, _):
            b, pp = lax.div(r, 2), lax.rem(r, 2)
            rows_at = pl.ds(pl.multiple_of(pp * cap, cap), cap)
            res = (oacc[b, rows_at, :] + hidden_times_down(recv[j, b, rows_at, :], last)).astype(BF16)
            own = (b >= 2) & (pp == 0)

            @pl.when(own)
            def _():
                back[j, lax.rem(b, 2), 0, 0:cap, :] = res

            @pl.when(jnp.logical_not(own))
            def _():
                recv[j, b, rows_at, :] = res

            @pl.when((r > 0) & (r != 5) & (r != 7))
            def _():
                ret_copy(index_of(r - 1)).start()

            return 0

        lax.fori_loop(0, 8, finish, 0)
        ret_copy(index_of(7)).start()
        if j == 0:
            pl.semaphore_signal(credit, inc=1, device_id=y_other)
            pl.semaphore_wait(credit, 1)
            for c in w_remote(1, last) + w_local(1, last):
                c.start()

    def combine(j, pp, mb):
        i = j * 8 + mb * 4 + pp
        ret_copy(i).wait_recv()

        @pl.when(pp == 1)
        def _():
            ret_copy(i + 2).wait_recv()

        base = ((j * 2 + pp) * 2 * cap).astype(F32)
        want = lax.broadcasted_iota(jnp.int32, (LANES, 2 * cap), 1).astype(F32) + base
        for g in range(groups):
            c_buf[g * LANES:(g + 1) * LANES, :] = jnp.where(col_buf[mb, :, g:g + 1] == want, 1.0, 0.0).astype(BF16)
        for blk in range(4):
            size = tok // 4
            picked = dot(c_buf[blk * size:(blk + 1) * size, :], back[j, mb, pp])
            for s in range(size // LANES):
                g = blk * (size // LANES) + s
                at = slice(g * LANES, (g + 1) * LANES)
                gate = col_buf[mb, :, groups + g:groups + g + 1]
                part = picked[s * LANES:(s + 1) * LANES, :]
                xbuf[mb, at, :] = (xbuf[mb, at, :].astype(F32) + gate * part).astype(BF16)

    def combine_step(n, pp):
        combine(lax.rem(lax.div(n, 2), 2), pp, lax.rem(n, 2))

    expert(0)

    def early(n, _):
        combine_step(n, jnp.int32(1))
        return 0

    lax.fori_loop(0, 4 * c_me, early, 0)
    expert(1)

    def late(n, _):
        combine_step(n, lax.div(n, 4))
        return 0

    total = 8 - 4 * c_me
    lax.fori_loop(0, total - 1, late, 0)
    outs = [pltpu.make_async_copy(xbuf.at[mb], y_hbm.at[mb], y_sem.at[mb]) for mb in range(n_mb)]
    outs[0].start()
    late(total - 1, 0)
    outs[1].start()

    for i in range(16):
        if i % 4 != 2:
            tok_copy(i).wait_send()
            ret_copy(i).wait_send()
    for c in outs:
        c.wait()


def solution(mesh):
    row_spec = P(None, ('rep', 'expert', 'data'), None)
    up_spec = P('expert', 'data', None)
    down_spec = P('expert', None, 'data')

    def per_device(x_loc, idx_loc, gate_loc, wg_loc, wu_loc, wd_loc):
        n_mb, tok, d_model = x_loc.shape
        n_loc, half, ff = wg_loc.shape
        n_exp = n_loc * mesh.shape['expert']
        n_top = idx_loc.shape[2]
        assert n_top == 1 and n_exp == 8 and n_mb == 2
        cap = 8 * ((5 * n_top * tok + 32 * n_exp - 1) // (32 * n_exp))
        fc = 256
        nf = ff // fc
        groups = tok // LANES
        hbm = pl.BlockSpec(memory_space=pl.ANY)
        vmem = pl.BlockSpec(memory_space=pltpu.VMEM)
        dma = pltpu.SemaphoreType.DMA
        return pl.pallas_call(
            functools.partial(moe_kernel, (cap, fc, nf)),
            out_shape=jax.ShapeDtypeStruct(x_loc.shape, BF16),
            in_specs=[vmem, vmem, hbm, hbm, hbm, hbm],
            out_specs=hbm,
            scratch_shapes=[
                pltpu.VMEM((n_mb, tok, d_model), BF16),
                pltpu.VMEM((16, cap, d_model), BF16),
                pltpu.VMEM((2, 4, 2 * cap, d_model), BF16),
                pltpu.VMEM((2, n_mb, 2, 2 * cap, d_model), BF16),
                pltpu.VMEM((4, 2 * cap, d_model), F32),
                pltpu.VMEM((nf, d_model, fc), BF16),
                pltpu.VMEM((nf, d_model, fc), BF16),
                pltpu.VMEM((nf, fc, d_model), BF16),
                pltpu.VMEM((cap, tok), BF16),
                pltpu.VMEM((tok, 2 * cap), BF16),
                pltpu.VMEM((n_mb, groups, LANES), F32),
                pltpu.VMEM((n_mb, LANES, LANES), F32),
                pltpu.VMEM((n_mb, LANES, LANES), F32),
                dma((n_mb,)), dma((n_mb,)),
                dma((16,)), dma((16,)), dma((16,)), dma((16,)),
                dma((nf, 3)), dma((nf, 3)), dma((nf, 3)),
                pltpu.SemaphoreType.REGULAR, pltpu.SemaphoreType.REGULAR,
            ],
            compiler_params=pltpu.CompilerParams(
                collective_id=0, has_side_effects=True, vmem_limit_bytes=64 * 1024 * 1024 - 65536),
        )(idx_loc.reshape(n_mb, groups, LANES), gate_loc.reshape(n_mb, groups, LANES), x_loc, wg_loc, wu_loc, wd_loc)

    return jax.shard_map(per_device, mesh=mesh, in_specs=(row_spec, row_spec, row_spec, up_spec, up_spec, down_spec),
                         out_specs=row_spec, check_vma=False)
```

```python
import functools

import jax
import jax.numpy as jnp
from jax import lax
from jax.experimental import pallas as pl
from jax.experimental.pallas import tpu as pltpu
from jax.sharding import PartitionSpec as P

F32 = jnp.float32
BF16 = jnp.bfloat16
LANES = 128


def dot(a, b):
    return jnp.dot(a, b, preferred_element_type=F32)


def moe_kernel(dims, ids_ref, gate_ref, x_hbm, wg_hbm, wu_hbm, wd_hbm, y_hbm,
               xbuf, send, recv, back, oacc, wg_buf, wu_buf, wd_buf, p_buf, c_buf, slot_buf, cat_buf, col_buf,
               x_sem, y_sem, tok_send, tok_recv, ret_send, ret_recv, w_send, w_recv, w_loc, credit, go):
    cap, fc, nf, early = dims
    n_mb, tok, d_model = xbuf.shape
    half = d_model // 2
    groups = tok // LANES
    q_me = lax.axis_index('expert')
    y_me = lax.axis_index('data')
    x_me, c_me = lax.div(q_me, 2), lax.rem(q_me, 2)
    is_a = c_me == 0
    is_b = c_me == 1

    def device(dx, dy, c):
        return {'expert': lax.rem(x_me + dx, 2) * 2 + c, 'data': lax.rem(y_me + dy, 2)}

    def piece(i):
        g = lax.div(i, 4)
        hi = 1 - lax.div(lax.rem(i, 4), 2)
        return g, hi, lax.rem(i, 2)

    def home_own(i):
        g, hi, _ = piece(i)
        return (hi == 0) & (((g >= 2) & is_a) | ((g == 1) & is_b))

    def slot_own(b, sub):
        hi = 1 - lax.div(lax.rem(b, 4), 2)
        return (hi == 0) & (sub == c_me) & (is_a | (b >= 4))

    def part(sub):
        return pl.ds(pl.multiple_of(sub * cap, cap), cap)

    def tok_copy(i):
        g, hi, mb = piece(i)
        dev = device(hi, jnp.where(g == 0, 1, 0), jnp.where(g >= 2, 0, 1))
        b = lax.rem(i, 8)
        return pltpu.make_async_remote_copy(send.at[i], recv.at[b, part(c_me), :], tok_send.at[i],
                                            tok_recv.at[b * 2 + c_me], device_id=dev)

    def tok_arrival(b, sub):
        return pltpu.make_async_remote_copy(send.at[0], recv.at[b, part(sub), :], tok_send.at[0],
                                            tok_recv.at[b * 2 + sub], device_id=device(1, 0, 0))

    def ret_copy(b, sub):
        g = (1 - c_me) * 2 + lax.div(b, 4)
        hi = 1 - lax.div(lax.rem(b, 4), 2)
        mb = lax.rem(b, 2)
        dev = device(hi, jnp.where(g == 0, 1, 0), sub)
        i = (1 - c_me) * 8 + b
        return pltpu.make_async_remote_copy(recv.at[b, part(sub), :], back.at[g, mb, part(hi), :],
                                            ret_send.at[b * 2 + sub], ret_recv.at[i], device_id=dev)

    def ret_arrival(i):
        g, hi, mb = piece(i)
        return pltpu.make_async_remote_copy(send.at[0], back.at[g, mb, part(hi), :], ret_send.at[0],
                                            ret_recv.at[i], device_id=device(1, 0, 0))

    y_other = {'data': 1 - y_me}
    my_half = pl.ds(pl.multiple_of(y_me * half, half), half)

    def w_parts(j, k):
        cols = pl.ds(pl.multiple_of(k * fc, fc), fc)
        return ((wg_hbm.at[j, :, cols], wg_buf.at[k, my_half, :], 0),
                (wu_hbm.at[j, :, cols], wu_buf.at[k, my_half, :], 1),
                (wd_hbm.at[j, cols, :], wd_buf.at[k, :, my_half], 2))

    def w_remote(j, k):
        return [pltpu.make_async_remote_copy(s, d, w_send.at[k, n], w_recv.at[k, n], device_id=y_other)
                for s, d, n in w_parts(j, k)]

    def w_local(j, k):
        return [pltpu.make_async_copy(s, d, w_loc.at[k, n]) for s, d, n in w_parts(j, k)]

    barrier = pltpu.get_barrier_semaphore()
    for n in range(1, 8):
        other = device(n // 4, (n // 2) % 2, lax.rem(c_me + n % 2, 2))
        pl.semaphore_signal(barrier, inc=1, device_id=other)
    pl.semaphore_wait(barrier, 7)

    j_out = jnp.where(is_a, 0, 1 - y_me)
    j_in = jnp.where(is_a, 0, y_me)

    def start_remote(k, _):
        for c in w_remote(j_out, k):
            c.start()
        return 0

    def start_local(k, _):
        for c in w_local(j_in, k):
            c.start()
        return 0

    lax.fori_loop(0, early * c_me, start_remote, 0)
    x_loads = [pltpu.make_async_copy(x_hbm.at[mb], xbuf.at[mb], x_sem.at[mb]) for mb in range(n_mb)]
    for c in x_loads:
        c.start()
    lax.fori_loop(0, nf, start_local, 0)

    masks = []
    for mb in range(n_mb):
        ids = ids_ref[mb]
        for e in range(8):
            masks.append((ids == e).astype(F32))
    stack = jnp.concatenate(masks, axis=0).astype(BF16)
    rows = stack.shape[0]
    lane_r = lax.broadcasted_iota(jnp.int32, (LANES, LANES), 0)
    lane_c = lax.broadcasted_iota(jnp.int32, (LANES, LANES), 1)
    upper = jnp.where(lane_r < lane_c, 1.0, 0.0).astype(BF16)
    row_r = lax.broadcasted_iota(jnp.int32, (rows, rows), 0)
    row_c = lax.broadcasted_iota(jnp.int32, (rows, rows), 1)
    first = row_r - lax.rem(row_r, groups)
    lower = jnp.where((row_c >= first) & (row_c < row_r), 1.0, 0.0).astype(BF16)
    ones = jnp.ones((LANES, LANES), BF16)
    prefix = dot(stack, upper) + dot(dot(lower, stack).astype(BF16), ones)
    cat_buf[...] = jnp.zeros_like(cat_buf)
    for mb in range(n_mb):
        place = jnp.full((groups, LANES), -1.0, F32)
        for e in range(8):
            r0 = (mb * 8 + e) * groups
            slot = prefix[r0:r0 + groups]
            x_e, c_e, j = e // 4, (e // 2) % 2, e % 2
            hi = lax.rem(x_me + x_e, 2)
            g = 1 - lax.rem(y_me + j, 2) if c_e else 2 + j
            base = ((g * 2 + hi) * cap).astype(F32)
            place = jnp.where((masks[mb * 8 + e] > 0.5) & (slot < float(cap)), base + slot, place)
        slot_buf[mb] = place
        cat_buf[mb, 0:groups, :] = place
        cat_buf[mb, groups:2 * groups, :] = gate_ref[mb]
        col_buf[mb] = cat_buf[mb].T

    for c in x_loads:
        c.wait()

    def dispatch(i, _):
        g, hi, mb = piece(i)
        base = ((g * 2 + hi) * cap).astype(F32)
        want = lax.broadcasted_iota(jnp.int32, (cap, LANES), 0).astype(F32) + base
        place = slot_buf[mb]
        for n in range(groups):
            p_buf[:, n * LANES:(n + 1) * LANES] = jnp.where(place[n:n + 1, :] == want, 1.0, 0.0).astype(BF16)
        out = dot(p_buf[...], xbuf[mb]).astype(BF16)
        own = home_own(i)

        @pl.when(own)
        def _():
            recv[lax.rem(i, 8), part(c_me), :] = out

        @pl.when(jnp.logical_not(own))
        def _():
            send[i] = out

        @pl.when((i > 0) & jnp.logical_not(home_own(i - 1)))
        def _():
            tok_copy(i - 1).start()

        return 0

    lax.fori_loop(0, 16, dispatch, 0)

    @pl.when(is_b)
    def _():
        tok_copy(15).start()

    def wait_tokens(b, _):
        for sub in range(2):
            @pl.when(jnp.logical_not(slot_own(b, sub)))
            def _():
                tok_arrival(b, sub).wait_recv()
        return 0

    def wait_weights(k):
        for c in w_local(0, k):
            c.wait()
        for c in w_remote(0, k):
            c.wait()

    def ffn(rows_in, k):
        gate_pre = dot(rows_in, wg_buf[k])
        up_pre = dot(rows_in, wu_buf[k])
        hidden = (gate_pre / (1.0 + jnp.exp(-gate_pre)) * up_pre).astype(BF16)
        return dot(hidden, wd_buf[k])

    def clear(b, _):
        oacc[b] = jnp.zeros_like(oacc[b])
        return 0

    def add_chunk(k, lo, hi):
        def block(b, _):
            oacc[b] += ffn(recv[b], k)
            return 0

        lax.fori_loop(lo, hi, block, 0)

    def finish(lo, hi):
        last = nf - 1

        def one(r, _):
            b, sub = lax.div(r, 2), lax.rem(r, 2)
            res = (oacc[b, part(sub), :] + ffn(recv[b, part(sub), :], last)).astype(BF16)
            own = slot_own(b, sub)

            @pl.when(own)
            def _():
                back[(1 - c_me) * 2 + lax.div(b, 4), lax.rem(b, 2), 0:cap, :] = res

            @pl.when(jnp.logical_not(own))
            def _():
                recv[b, part(sub), :] = res

            before = r - 1

            @pl.when((r > lo * 2) & jnp.logical_not(slot_own(lax.div(before, 2), lax.rem(before, 2))))
            def _():
                ret_copy(lax.div(before, 2), lax.rem(before, 2)).start()

            return 0

        lax.fori_loop(lo * 2, hi * 2, one, 0)

    def combine(g, mb):
        for hi in range(2):
            i = g * 4 + (1 - hi) * 2 + mb

            @pl.when(jnp.logical_not(home_own(i)))
            def _():
                ret_arrival(i).wait_recv()

        want = lax.broadcasted_iota(jnp.int32, (LANES, 2 * cap), 1).astype(F32) + (g * 2 * cap).astype(F32)
        size = c_buf.shape[0]
        for blk in range(tok // size):
            for s in range(size // LANES):
                n = blk * (size // LANES) + s
                c_buf[s * LANES:(s + 1) * LANES, :] = jnp.where(col_buf[mb, :, n:n + 1] == want, 1.0, 0.0).astype(BF16)
            picked = dot(c_buf[...], back[g, mb])
            for s in range(size // LANES):
                n = blk * (size // LANES) + s
                at = slice(n * LANES, (n + 1) * LANES)
                gate = col_buf[mb, :, groups + n:groups + n + 1]
                xbuf[mb, at, :] = (xbuf[mb, at, :].astype(F32) + gate * picked[s * LANES:(s + 1) * LANES, :]).astype(BF16)

    @pl.when(is_a)
    def _():
        pl.semaphore_wait(go, 1)
        lax.fori_loop(0, nf, start_remote, 0)

        def expert(j, _):
            lo, hi = j * 4, j * 4 + 4
            lax.fori_loop(lo, hi, clear, 0)
            lax.fori_loop(lo, hi, wait_tokens, 0)

            def refill(k):
                @pl.when(j == 0)
                def _():
                    pl.semaphore_signal(credit, inc=1, device_id=y_other)
                    pl.semaphore_wait(credit, 1)
                    for c in w_remote(1, k) + w_local(1, k):
                        c.start()

            def chunk(k, _):
                wait_weights(k)
                add_chunk(k, lo, hi)
                refill(k)

                @pl.when((k == nf - 3) & (j == 1))
                def _():
                    pl.semaphore_signal(go, inc=1, device_id=device(0, 0, 1))

                return 0

            lax.fori_loop(0, nf - 1, chunk, 0)
            wait_weights(nf - 1)
            finish(lo, hi)
            ret_copy(hi - 1, 1).start()
            refill(nf - 1)
            return 0

        lax.fori_loop(0, 2, expert, 0)

    def combine_both(g):
        def step(mb, _):
            combine(g, mb)
            return 0

        lax.fori_loop(0, n_mb, step, 0)

    @pl.when(is_b)
    def _():
        for c in w_remote(j_out, early - 3):
            c.wait_send()
        pl.semaphore_signal(go, inc=1, device_id=device(0, 0, 0))
        lax.fori_loop(0, 8, clear, 0)
        lax.fori_loop(0, 8, wait_tokens, 0)

        def chunk(k, _):
            for c in w_local(0, k):
                c.wait()
            for c in w_remote(0, k):
                c.wait_recv()

            @pl.when(k != early - 3)
            def _():
                for c in w_remote(0, k):
                    c.wait_send()

            @pl.when(k < nf - 1)
            def _():
                add_chunk(k, 0, 8)

            @pl.when(k == early - 1)
            def _():
                combine_both(jnp.int32(2))
                pl.semaphore_wait(go, 1)
                lax.fori_loop(early, nf, start_remote, 0)

            return 0

        lax.fori_loop(0, nf, chunk, 0)
        finish(0, 8)

    def late(n, _):
        g = lax.rem(lax.div(n, 2) + 2, 4)
        combine(g, lax.rem(n, 2))
        return 0

    lax.fori_loop(2 * c_me, 7, late, 0)
    outs = [pltpu.make_async_copy(xbuf.at[mb], y_hbm.at[mb], y_sem.at[mb]) for mb in range(n_mb)]
    outs[0].start()
    late(jnp.int32(7), 0)
    outs[1].start()

    def drain(i, _):
        @pl.when(jnp.logical_not(home_own(i)))
        def _():
            tok_copy(i).wait_send()

        b, sub = lax.div(i, 2), lax.rem(i, 2)

        @pl.when(jnp.logical_not(slot_own(b, sub)))
        def _():
            ret_copy(b, sub).wait_send()

        return 0

    lax.fori_loop(0, 16, drain, 0)
    for c in outs:
        c.wait()


def solution(mesh):
    row_spec = P(None, ('rep', 'expert', 'data'), None)
    up_spec = P('expert', 'data', None)
    down_spec = P('expert', None, 'data')

    def per_device(x_loc, idx_loc, gate_loc, wg_loc, wu_loc, wd_loc):
        n_mb, tok, d_model = x_loc.shape
        n_loc, half, ff = wg_loc.shape
        n_exp = n_loc * mesh.shape['expert']
        n_top = idx_loc.shape[2]
        assert n_top == 1 and n_exp == 8 and n_mb == 2
        cap = 8 * ((5 * n_top * tok + 32 * n_exp - 1) // (32 * n_exp))
        fc = 256
        nf = ff // fc
        early = 9
        groups = tok // LANES
        hbm = pl.BlockSpec(memory_space=pl.ANY)
        vmem = pl.BlockSpec(memory_space=pltpu.VMEM)
        dma = pltpu.SemaphoreType.DMA
        return pl.pallas_call(
            functools.partial(moe_kernel, (cap, fc, nf, early)),
            out_shape=jax.ShapeDtypeStruct(x_loc.shape, BF16),
            in_specs=[vmem, vmem, hbm, hbm, hbm, hbm],
            out_specs=hbm,
            scratch_shapes=[
                pltpu.VMEM((n_mb, tok, d_model), BF16),
                pltpu.VMEM((16, cap, d_model), BF16),
                pltpu.VMEM((8, 2 * cap, d_model), BF16),
                pltpu.VMEM((4, n_mb, 2 * cap, d_model), BF16),
                pltpu.VMEM((8, 2 * cap, d_model), F32),
                pltpu.VMEM((nf, d_model, fc), BF16),
                pltpu.VMEM((nf, d_model, fc), BF16),
                pltpu.VMEM((nf, fc, d_model), BF16),
                pltpu.VMEM((cap, tok), BF16),
                pltpu.VMEM((512, 2 * cap), BF16),
                pltpu.VMEM((n_mb, groups, LANES), F32),
                pltpu.VMEM((n_mb, LANES, LANES), F32),
                pltpu.VMEM((n_mb, LANES, LANES), F32),
                dma((n_mb,)), dma((n_mb,)),
                dma((16,)), dma((16,)), dma((16,)), dma((16,)),
                dma((nf, 3)), dma((nf, 3)), dma((nf, 3)),
                pltpu.SemaphoreType.REGULAR, pltpu.SemaphoreType.REGULAR,
            ],
            compiler_params=pltpu.CompilerParams(
                collective_id=0, has_side_effects=True, vmem_limit_bytes=64 * 1024 * 1024 - 65536),
        )(idx_loc.reshape(n_mb, groups, LANES), gate_loc.reshape(n_mb, groups, LANES), x_loc, wg_loc, wu_loc, wd_loc)

    return jax.shard_map(per_device, mesh=mesh, in_specs=(row_spec, row_spec, row_spec, up_spec, up_spec, down_spec),
                         out_specs=row_spec, check_vma=False)
```

```python
import functools

import jax
import jax.numpy as jnp
from jax import lax
from jax.experimental import pallas as pl
from jax.experimental.pallas import tpu as pltpu
from jax.sharding import PartitionSpec as P

F32 = jnp.float32
BF16 = jnp.bfloat16
LANES = 128
SIGNAL_AFTER = 1


def dot(a, b):
    return jnp.dot(a, b, preferred_element_type=F32)


def moe_kernel(dims, ids_ref, gate_ref, x_hbm, wg_hbm, wu_hbm, wd_hbm, y_hbm,
               xbuf, send, recv, back, oacc, wg_buf, wu_buf, wd_buf, p_buf, c_buf, slot_buf, cat_buf, col_buf,
               x_sem, y_sem, tok_send, tok_recv, ret_send, ret_recv, w_send, w_recv, w_loc, credit, go):
    cap, fc, nf, early = dims
    n_mb, tok, d_model = xbuf.shape
    half = d_model // 2
    groups = tok // LANES
    q_me = lax.axis_index('expert')
    y_me = lax.axis_index('data')
    x_me, c_me = lax.div(q_me, 2), lax.rem(q_me, 2)
    is_a = c_me == 0
    is_b = c_me == 1

    def device(dx, dy, c):
        return {'expert': lax.rem(x_me + dx, 2) * 2 + c, 'data': lax.rem(y_me + dy, 2)}

    def piece(i):
        g = lax.div(i, 4)
        hi = 1 - lax.div(lax.rem(i, 4), 2)
        return g, hi, lax.rem(i, 2)

    def home_own(i):
        g, hi, _ = piece(i)
        return (hi == 0) & (((g >= 2) & is_a) | ((g == 1) & is_b))

    def slot_own(b, sub):
        hi = 1 - lax.div(lax.rem(b, 4), 2)
        return (hi == 0) & (sub == c_me) & (is_a | (b >= 4))

    def part(sub):
        return pl.ds(pl.multiple_of(sub * cap, cap), cap)

    def tok_copy(i):
        g, hi, mb = piece(i)
        dev = device(hi, jnp.where(g == 0, 1, 0), jnp.where(g >= 2, 0, 1))
        b = lax.rem(i, 8)
        return pltpu.make_async_remote_copy(send.at[i], recv.at[b, part(c_me), :], tok_send.at[i],
                                            tok_recv.at[b * 2 + c_me], device_id=dev)

    def tok_arrival(b, sub):
        return pltpu.make_async_remote_copy(send.at[0], recv.at[b, part(sub), :], tok_send.at[0],
                                            tok_recv.at[b * 2 + sub], device_id=device(1, 0, 0))

    def ret_copy(b, sub):
        g = (1 - c_me) * 2 + lax.div(b, 4)
        hi = 1 - lax.div(lax.rem(b, 4), 2)
        mb = lax.rem(b, 2)
        dev = device(hi, jnp.where(g == 0, 1, 0), sub)
        i = (1 - c_me) * 8 + b
        return pltpu.make_async_remote_copy(recv.at[b, part(sub), :], back.at[g, mb, part(hi), :],
                                            ret_send.at[b * 2 + sub], ret_recv.at[i], device_id=dev)

    def ret_arrival(i):
        g, hi, mb = piece(i)
        return pltpu.make_async_remote_copy(send.at[0], back.at[g, mb, part(hi), :], ret_send.at[0],
                                            ret_recv.at[i], device_id=device(1, 0, 0))

    y_other = {'data': 1 - y_me}
    my_half = pl.ds(pl.multiple_of(y_me * half, half), half)

    def w_parts(j, k):
        cols = pl.ds(pl.multiple_of(k * fc, fc), fc)
        return ((wg_hbm.at[j, :, cols], wg_buf.at[k, my_half, :], 0),
                (wu_hbm.at[j, :, cols], wu_buf.at[k, my_half, :], 1),
                (wd_hbm.at[j, cols, :], wd_buf.at[k, :, my_half], 2))

    def w_remote(j, k):
        return [pltpu.make_async_remote_copy(s, d, w_send.at[k, n], w_recv.at[k, n], device_id=y_other)
                for s, d, n in w_parts(j, k)]

    def w_local(j, k):
        return [pltpu.make_async_copy(s, d, w_loc.at[k, n]) for s, d, n in w_parts(j, k)]

    barrier = pltpu.get_barrier_semaphore()
    for n in range(1, 8):
        other = device(n // 4, (n // 2) % 2, lax.rem(c_me + n % 2, 2))
        pl.semaphore_signal(barrier, inc=1, device_id=other)
    pl.semaphore_wait(barrier, 7)

    j_out = jnp.where(is_a, 0, 1 - y_me)
    j_in = jnp.where(is_a, 0, y_me)

    def start_remote(k, _):
        for c in w_remote(j_out, k):
            c.start()
        return 0

    def start_local(k, _):
        for c in w_local(j_in, k):
            c.start()
        return 0

    lax.fori_loop(0, early * c_me, start_remote, 0)
    x_loads = [pltpu.make_async_copy(x_hbm.at[mb], xbuf.at[mb], x_sem.at[mb]) for mb in range(n_mb)]
    for c in x_loads:
        c.start()
    lax.fori_loop(0, nf, start_local, 0)

    masks = []
    for mb in range(n_mb):
        ids = ids_ref[mb]
        for e in range(8):
            masks.append((ids == e).astype(F32))
    stack = jnp.concatenate(masks, axis=0).astype(BF16)
    rows = stack.shape[0]
    lane_r = lax.broadcasted_iota(jnp.int32, (LANES, LANES), 0)
    lane_c = lax.broadcasted_iota(jnp.int32, (LANES, LANES), 1)
    upper = jnp.where(lane_r < lane_c, 1.0, 0.0).astype(BF16)
    row_r = lax.broadcasted_iota(jnp.int32, (rows, rows), 0)
    row_c = lax.broadcasted_iota(jnp.int32, (rows, rows), 1)
    first = row_r - lax.rem(row_r, groups)
    lower = jnp.where((row_c >= first) & (row_c < row_r), 1.0, 0.0).astype(BF16)
    ones = jnp.ones((LANES, LANES), BF16)
    prefix = dot(stack, upper) + dot(dot(lower, stack).astype(BF16), ones)
    cat_buf[...] = jnp.zeros_like(cat_buf)
    for mb in range(n_mb):
        place = jnp.full((groups, LANES), -1.0, F32)
        for e in range(8):
            r0 = (mb * 8 + e) * groups
            slot = prefix[r0:r0 + groups]
            x_e, c_e, j = e // 4, (e // 2) % 2, e % 2
            hi = lax.rem(x_me + x_e, 2)
            g = 1 - lax.rem(y_me + j, 2) if c_e else 2 + j
            base = ((g * 2 + hi) * cap).astype(F32)
            place = jnp.where((masks[mb * 8 + e] > 0.5) & (slot < float(cap)), base + slot, place)
        slot_buf[mb] = place
        cat_buf[mb, 0:groups, :] = place
        cat_buf[mb, groups:2 * groups, :] = gate_ref[mb]
        col_buf[mb] = cat_buf[mb].T

    for c in x_loads:
        c.wait()

    def dispatch(i, _):
        g, hi, mb = piece(i)
        base = ((g * 2 + hi) * cap).astype(F32)
        want = lax.broadcasted_iota(jnp.int32, (cap, LANES), 0).astype(F32) + base
        place = slot_buf[mb]
        out = None
        for h in range(2):
            for n in range(groups // 2):
                at = h * (groups // 2) + n
                p_buf[:, n * LANES:(n + 1) * LANES] = jnp.where(place[at:at + 1, :] == want, 1.0, 0.0).astype(BF16)
            picked = dot(p_buf[...], xbuf[mb, h * (tok // 2):(h + 1) * (tok // 2), :])
            out = picked if h == 0 else (out + picked).astype(BF16)
        own = home_own(i)

        @pl.when(own)
        def _():
            recv[lax.rem(i, 8), part(c_me), :] = out

        @pl.when(jnp.logical_not(own))
        def _():
            send[i] = out

        @pl.when((i > 0) & jnp.logical_not(home_own(i - 1)))
        def _():
            tok_copy(i - 1).start()

        return 0

    lax.fori_loop(0, 16, dispatch, 0)

    @pl.when(is_b)
    def _():
        tok_copy(15).start()

    def wait_tokens(b, _):
        for sub in range(2):
            @pl.when(jnp.logical_not(slot_own(b, sub)))
            def _():
                tok_arrival(b, sub).wait_recv()
        return 0

    def wait_weights(k):
        for local, remote in zip(w_local(0, k), w_remote(0, k)):
            local.wait()
            remote.wait()

    def pre(rows_in, k):
        return dot(rows_in, wg_buf[k]), dot(rows_in, wu_buf[k])

    def post(gate_up, k):
        gate_pre, up_pre = gate_up
        hidden = (gate_pre / (1.0 + jnp.exp(-gate_pre)) * up_pre).astype(BF16)
        return dot(hidden, wd_buf[k])

    def clear(b, _):
        oacc[b] = jnp.zeros_like(oacc[b])
        return 0

    def add_chunk(k, lo, hi):
        def pair(t, _):
            both = [(t * 2 + n, pre(recv[t * 2 + n], k)) for n in range(2)]
            for b, pre_b in both:
                oacc[b] += post(pre_b, k)
            return 0

        lax.fori_loop(lax.div(lo, 2), lax.div(hi, 2), pair, 0)

    def finish(lo, hi):
        last = nf - 1

        def slot_of(r):
            t = lax.div(r, 2)
            straight = 2 + lax.rem(t, 2) * 2 + lax.div(t, 2)
            return jnp.where(is_a | (t >= 6), t, jnp.where(t < 4, straight, t - 4)), lax.rem(r, 2)

        def one(r, _):
            b, sub = slot_of(r)
            res = (oacc[b, part(sub), :] + post(pre(recv[b, part(sub), :], last), last)).astype(BF16)
            own = slot_own(b, sub)

            @pl.when(own)
            def _():
                back[(1 - c_me) * 2 + lax.div(b, 4), lax.rem(b, 2), 0:cap, :] = res

            @pl.when(jnp.logical_not(own))
            def _():
                recv[b, part(sub), :] = res

            b_old, sub_old = slot_of(r - 1)

            @pl.when((r > lo * 2) & jnp.logical_not(slot_own(b_old, sub_old)))
            def _():
                ret_copy(b_old, sub_old).start()

            return 0

        lax.fori_loop(lo * 2, hi * 2, one, 0)

    def combine(g, mb):
        for hi in range(2):
            i = g * 4 + (1 - hi) * 2 + mb

            @pl.when(jnp.logical_not(home_own(i)))
            def _():
                ret_arrival(i).wait_recv()

        want = lax.broadcasted_iota(jnp.int32, (LANES, 2 * cap), 1).astype(F32) + (g * 2 * cap).astype(F32)
        size = c_buf.shape[0]
        for blk in range(tok // size):
            for s in range(size // LANES):
                n = blk * (size // LANES) + s
                c_buf[s * LANES:(s + 1) * LANES, :] = jnp.where(col_buf[mb, :, n:n + 1] == want, 1.0, 0.0).astype(BF16)
            picked = dot(c_buf[...], back[g, mb])
            for s in range(size // LANES):
                n = blk * (size // LANES) + s
                at = slice(n * LANES, (n + 1) * LANES)
                gate = col_buf[mb, :, groups + n:groups + n + 1]
                xbuf[mb, at, :] = (xbuf[mb, at, :].astype(F32) + gate * picked[s * LANES:(s + 1) * LANES, :]).astype(BF16)

    @pl.when(is_a)
    def _():
        pl.semaphore_wait(go, 1)
        lax.fori_loop(0, nf, start_remote, 0)

        def expert(j, _):
            lo, hi = j * 4, j * 4 + 4
            lax.fori_loop(lo, hi, clear, 0)
            lax.fori_loop(lo, hi, wait_tokens, 0)

            def refill(k):
                @pl.when(j == 0)
                def _():
                    pl.semaphore_signal(credit, inc=1, device_id=y_other)
                    pl.semaphore_wait(credit, 1)
                    for c in w_remote(1, k) + w_local(1, k):
                        c.start()

            def chunk(k, _):
                wait_weights(k)
                add_chunk(k, lo, hi)
                refill(k)

                return 0

            lax.fori_loop(0, nf - 1, chunk, 0)
            last_parts = list(zip(w_local(0, nf - 1), w_remote(0, nf - 1)))
            for n, (local, remote) in enumerate(last_parts):
                local.wait()
                remote.wait()
                if n == SIGNAL_AFTER:
                    @pl.when(j == 1)
                    def _():
                        pl.semaphore_signal(go, inc=1, device_id=device(0, 0, 1))

            finish(lo, hi)
            ret_copy(hi - 1, 1).start()
            refill(nf - 1)
            return 0

        lax.fori_loop(0, 2, expert, 0)

    def combine_both(g):
        def step(mb, _):
            combine(g, mb)
            return 0

        lax.fori_loop(0, n_mb, step, 0)

    @pl.when(is_b)
    def _():
        for c in w_remote(j_out, early - 3):
            c.wait_send()
        pl.semaphore_signal(go, inc=1, device_id=device(0, 0, 0))
        lax.fori_loop(0, 8, clear, 0)
        lax.fori_loop(0, 8, wait_tokens, 0)

        def chunk(k, _):
            for c in w_local(0, k):
                c.wait()
            for c in w_remote(0, k):
                c.wait_recv()

            @pl.when(k != early - 3)
            def _():
                for c in w_remote(0, k):
                    c.wait_send()

            @pl.when(k < nf - 1)
            def _():
                add_chunk(k, jnp.int32(0), jnp.int32(8))

            @pl.when(k == early - 1)
            def _():
                combine_both(jnp.int32(2))
                pl.semaphore_wait(go, 1)
                lax.fori_loop(early, nf, start_remote, 0)

            return 0

        lax.fori_loop(0, nf, chunk, 0)
        finish(0, 8)

    def late(n, _):
        pair = lax.div(n, 2)
        g = jnp.where(pair < 2, pair + 2, 3 - pair)
        combine(g, lax.rem(n, 2))
        return 0

    lax.fori_loop(2 * c_me, 7, late, 0)
    outs = [pltpu.make_async_copy(xbuf.at[mb], y_hbm.at[mb], y_sem.at[mb]) for mb in range(n_mb)]
    outs[0].start()
    late(jnp.int32(7), 0)
    outs[1].start()

    def drain(i, _):
        @pl.when(jnp.logical_not(home_own(i)))
        def _():
            tok_copy(i).wait_send()

        b, sub = lax.div(i, 2), lax.rem(i, 2)

        @pl.when(jnp.logical_not(slot_own(b, sub)))
        def _():
            ret_copy(b, sub).wait_send()

        return 0

    lax.fori_loop(0, 16, drain, 0)
    for c in outs:
        c.wait()


def solution(mesh):
    row_spec = P(None, ('rep', 'expert', 'data'), None)
    up_spec = P('expert', 'data', None)
    down_spec = P('expert', None, 'data')

    def per_device(x_loc, idx_loc, gate_loc, wg_loc, wu_loc, wd_loc):
        n_mb, tok, d_model = x_loc.shape
        n_loc, half, ff = wg_loc.shape
        n_exp = n_loc * mesh.shape['expert']
        n_top = idx_loc.shape[2]
        assert n_top == 1 and n_exp == 8 and n_mb == 2
        cap = 8 * ((5 * n_top * tok + 32 * n_exp - 1) // (32 * n_exp))
        fc = 256
        nf = ff // fc
        early = 9
        groups = tok // LANES
        hbm = pl.BlockSpec(memory_space=pl.ANY)
        vmem = pl.BlockSpec(memory_space=pltpu.VMEM)
        dma = pltpu.SemaphoreType.DMA
        return pl.pallas_call(
            functools.partial(moe_kernel, (cap, fc, nf, early)),
            out_shape=jax.ShapeDtypeStruct(x_loc.shape, BF16),
            in_specs=[vmem, vmem, hbm, hbm, hbm, hbm],
            out_specs=hbm,
            scratch_shapes=[
                pltpu.VMEM((n_mb, tok, d_model), BF16),
                pltpu.VMEM((16, cap, d_model), BF16),
                pltpu.VMEM((8, 2 * cap, d_model), BF16),
                pltpu.VMEM((4, n_mb, 2 * cap, d_model), BF16),
                pltpu.VMEM((8, 2 * cap, d_model), F32),
                pltpu.VMEM((nf, d_model, fc), BF16),
                pltpu.VMEM((nf, d_model, fc), BF16),
                pltpu.VMEM((nf, fc, d_model), BF16),
                pltpu.VMEM((cap, tok // 2), BF16),
                pltpu.VMEM((512, 2 * cap), BF16),
                pltpu.VMEM((n_mb, groups, LANES), F32),
                pltpu.VMEM((n_mb, LANES, LANES), F32),
                pltpu.VMEM((n_mb, LANES, LANES), F32),
                dma((n_mb,)), dma((n_mb,)),
                dma((16,)), dma((16,)), dma((16,)), dma((16,)),
                dma((nf, 3)), dma((nf, 3)), dma((nf, 3)),
                pltpu.SemaphoreType.REGULAR, pltpu.SemaphoreType.REGULAR,
            ],
            compiler_params=pltpu.CompilerParams(
                collective_id=0, has_side_effects=True, vmem_limit_bytes=64 * 1024 * 1024 - 65536),
        )(idx_loc.reshape(n_mb, groups, LANES), gate_loc.reshape(n_mb, groups, LANES), x_loc, wg_loc, wu_loc, wd_loc)

    return jax.shard_map(per_device, mesh=mesh, in_specs=(row_spec, row_spec, row_spec, up_spec, up_spec, down_spec),
                         out_specs=row_spec, check_vma=False)
```

```python
import functools

import jax
import jax.numpy as jnp
from jax import lax
from jax.experimental import pallas as pl
from jax.experimental.pallas import tpu as pltpu
from jax.sharding import PartitionSpec as P

F32 = jnp.float32
BF16 = jnp.bfloat16
LANES = 128
SIGNAL_AFTER = 1


def dot(a, b):
    return jnp.dot(a, b, preferred_element_type=F32)


def moe_kernel(dims, ids_ref, gate_ref, x_hbm, wg_hbm, wu_hbm, wd_hbm, y_hbm, col_hbm, tail_hbm,
               xbuf, send, recv, back, oacc, wg_buf, wu_buf, wd_buf, p_buf, c_buf, slot_buf, cat_buf, col_buf,
               x_sem, y_sem, col_sem, tok_send, tok_recv, ret_send, ret_recv, w_send, w_recv, w_loc, credit, go):
    cap, fc, nf, early = dims
    n_mb, tok, d_model = xbuf.shape
    half = d_model // 2
    groups = tok // LANES
    q_me = lax.axis_index('expert')
    y_me = lax.axis_index('data')
    x_me, c_me = lax.div(q_me, 2), lax.rem(q_me, 2)
    is_a = c_me == 0
    is_b = c_me == 1

    def device(dx, dy, c):
        return {'expert': lax.rem(x_me + dx, 2) * 2 + c, 'data': lax.rem(y_me + dy, 2)}

    def piece(i):
        g = lax.div(i, 4)
        hi = 1 - lax.div(lax.rem(i, 4), 2)
        return g, hi, lax.rem(i, 2)

    def home_own(i):
        g, hi, _ = piece(i)
        return (hi == 0) & (((g >= 2) & is_a) | ((g == 1) & is_b))

    def slot_own(b, sub):
        hi = 1 - lax.div(lax.rem(b, 4), 2)
        return (hi == 0) & (sub == c_me) & (is_a | (b >= 4))

    def part(sub):
        return pl.ds(pl.multiple_of(sub * cap, cap), cap)

    def send_at(i):
        return jnp.where(i < 10, i, jnp.where(i < 12, i - 4, i - 2))

    def tok_copy(i):
        g, hi, mb = piece(i)
        dev = device(hi, jnp.where(g == 0, 1, 0), jnp.where(g >= 2, 0, 1))
        b = lax.rem(i, 8)
        return pltpu.make_async_remote_copy(send.at[send_at(i)], recv.at[b, part(c_me), :], tok_send.at[i],
                                            tok_recv.at[b * 2 + c_me], device_id=dev)

    def tok_arrival(b, sub):
        return pltpu.make_async_remote_copy(send.at[0], recv.at[b, part(sub), :], tok_send.at[0],
                                            tok_recv.at[b * 2 + sub], device_id=device(1, 0, 0))

    def ret_copy(b, sub, tail=False):
        g = (1 - c_me) * 2 + lax.div(b, 4)
        hi = 1 - lax.div(lax.rem(b, 4), 2)
        mb = lax.rem(b, 2)
        dev = device(hi, jnp.where(g == 0, 1, 0), sub)
        i = (1 - c_me) * 8 + b
        dst = tail_hbm if tail else back.at[g, mb, part(hi), :]
        return pltpu.make_async_remote_copy(recv.at[b, part(sub), :], dst,
                                            ret_send.at[b * 2 + sub], ret_recv.at[i], device_id=dev)

    def ret_do(b, sub, what):
        tail = is_b & (b == 1)

        @pl.when(tail)
        def _():
            what(ret_copy(b, sub, True))

        @pl.when(jnp.logical_not(tail))
        def _():
            what(ret_copy(b, sub))

    def ret_arrival(i):
        g, hi, mb = piece(i)
        return pltpu.make_async_remote_copy(send.at[0], back.at[g, mb, part(hi), :], ret_send.at[0],
                                            ret_recv.at[i], device_id=device(1, 0, 0))

    y_other = {'data': 1 - y_me}
    my_half = pl.ds(pl.multiple_of(y_me * half, half), half)

    def w_parts(j, k):
        cols = pl.ds(pl.multiple_of(k * fc, fc), fc)
        return ((wg_hbm.at[j, :, cols], wg_buf.at[k, my_half, :], 0),
                (wu_hbm.at[j, :, cols], wu_buf.at[k, my_half, :], 1),
                (wd_hbm.at[j, cols, :], wd_buf.at[k, :, my_half], 2))

    def w_remote(j, k):
        return [pltpu.make_async_remote_copy(s, d, w_send.at[k, n], w_recv.at[k, n], device_id=y_other)
                for s, d, n in w_parts(j, k)]

    def w_local(j, k):
        return [pltpu.make_async_copy(s, d, w_loc.at[k, n]) for s, d, n in w_parts(j, k)]

    barrier = pltpu.get_barrier_semaphore()
    for n in range(1, 8):
        other = device(n // 4, (n // 2) % 2, lax.rem(c_me + n % 2, 2))
        pl.semaphore_signal(barrier, inc=1, device_id=other)
    pl.semaphore_wait(barrier, 7)

    j_out = jnp.where(is_a, 0, 1 - y_me)
    j_in = jnp.where(is_a, 0, y_me)

    def start_remote(k, _):
        for c in w_remote(j_out, k):
            c.start()
        return 0

    def start_local(k, _):
        for c in w_local(j_in, k):
            c.start()
        return 0

    lax.fori_loop(0, early * c_me, start_remote, 0)
    x_loads = [pltpu.make_async_copy(x_hbm.at[mb], xbuf.at[mb], x_sem.at[mb]) for mb in range(n_mb)]
    for c in x_loads:
        c.start()
    lax.fori_loop(0, nf, start_local, 0)

    masks = []
    for mb in range(n_mb):
        ids = ids_ref[mb]
        for e in range(8):
            masks.append((ids == e).astype(F32))
    stack = jnp.concatenate(masks, axis=0).astype(BF16)
    rows = stack.shape[0]
    lane_r = lax.broadcasted_iota(jnp.int32, (LANES, LANES), 0)
    lane_c = lax.broadcasted_iota(jnp.int32, (LANES, LANES), 1)
    upper = jnp.where(lane_r < lane_c, 1.0, 0.0).astype(BF16)
    row_r = lax.broadcasted_iota(jnp.int32, (rows, rows), 0)
    row_c = lax.broadcasted_iota(jnp.int32, (rows, rows), 1)
    first = row_r - lax.rem(row_r, groups)
    lower = jnp.where((row_c >= first) & (row_c < row_r), 1.0, 0.0).astype(BF16)
    ones = jnp.ones((LANES, LANES), BF16)
    prefix = dot(stack, upper) + dot(dot(lower, stack).astype(BF16), ones)
    cat_buf[...] = jnp.zeros_like(cat_buf)
    for mb in range(n_mb):
        place = jnp.full((groups, LANES), -1.0, F32)
        for e in range(8):
            r0 = (mb * 8 + e) * groups
            slot = prefix[r0:r0 + groups]
            x_e, c_e, j = e // 4, (e // 2) % 2, e % 2
            hi = lax.rem(x_me + x_e, 2)
            g = 1 - lax.rem(y_me + j, 2) if c_e else 2 + j
            base = ((g * 2 + hi) * cap).astype(F32)
            place = jnp.where((masks[mb * 8 + e] > 0.5) & (slot < float(cap)), base + slot, place)
        slot_buf[mb] = place
        cat_buf[mb, 0:groups, :] = place
        cat_buf[mb, groups:2 * groups, :] = gate_ref[mb]
        col_buf[mb] = cat_buf[mb].T

    for c in x_loads:
        c.wait()

    def dispatch(i, _):
        g, hi, mb = piece(i)
        base = ((g * 2 + hi) * cap).astype(F32)
        want = lax.broadcasted_iota(jnp.int32, (cap, LANES), 0).astype(F32) + base
        place = slot_buf[mb]
        out = None
        for h in range(2):
            for n in range(groups // 2):
                at = h * (groups // 2) + n
                p_buf[:, n * LANES:(n + 1) * LANES] = jnp.where(place[at:at + 1, :] == want, 1.0, 0.0).astype(BF16)
            picked = dot(p_buf[...], xbuf[mb, h * (tok // 2):(h + 1) * (tok // 2), :])
            out = picked if h == 0 else (out + picked).astype(BF16)
        own = home_own(i)

        @pl.when(own)
        def _():
            recv[lax.rem(i, 8), part(c_me), :] = out

        @pl.when(jnp.logical_not(own))
        def _():
            send[send_at(i)] = out

        @pl.when((i > 0) & jnp.logical_not(home_own(i - 1)))
        def _():
            tok_copy(i - 1).start()

        return 0

    lax.fori_loop(0, 16, dispatch, 0)

    @pl.when(is_b)
    def _():
        tok_copy(15).start()

    def wait_tokens(b, _):
        for sub in range(2):
            @pl.when(jnp.logical_not(slot_own(b, sub)))
            def _():
                tok_arrival(b, sub).wait_recv()
        return 0

    def wait_weights(k):
        for local, remote in zip(w_local(0, k), w_remote(0, k)):
            local.wait()
            remote.wait()

    def pre(rows_in, k):
        return dot(rows_in, wg_buf[k]), dot(rows_in, wu_buf[k])

    def post(gate_up, k):
        gate_pre, up_pre = gate_up
        hidden = (gate_pre / (1.0 + jnp.exp(-gate_pre)) * up_pre).astype(BF16)
        return dot(hidden, wd_buf[k])

    def clear(b, _):
        oacc[b] = jnp.zeros_like(oacc[b])
        return 0

    def add_chunk(k, lo, hi):
        def pair(p, _):
            one = jnp.where(is_a, p * 2, jnp.where(p < 2, p * 6, p))
            two = jnp.where(is_a | (p < 2), one + 1, p + 2)
            both = [(b, pre(recv[b], k)) for b in (one, two)]
            for b, pre_b in both:
                oacc[b] += post(pre_b, k)
            return 0

        lax.fori_loop(lo, hi, pair, 0)

    def slot_of(r):
        t = lax.div(r, 2)
        straight = 2 + lax.rem(t, 2) * 2 + lax.div(t, 2)
        return jnp.where(is_a | (t >= 6), t, jnp.where(t < 4, straight, t - 4)), lax.rem(r, 2)

    def finish(start, lo, hi, chunks):
        def one(r, _):
            b_old, sub_old = slot_of(r - 1)

            @pl.when((r > start) & jnp.logical_not(slot_own(b_old, sub_old)))
            def _():
                ret_do(b_old, sub_old, lambda c: c.start())

            b, sub = slot_of(r)
            rows_in = recv[b, part(sub), :]
            total = oacc[b, part(sub), :]
            for k in chunks:
                total = total + post(pre(rows_in, k), k)
            res = total.astype(BF16)
            own = slot_own(b, sub)

            @pl.when(own)
            def _():
                back[(1 - c_me) * 2 + lax.div(b, 4), lax.rem(b, 2), 0:cap, :] = res

            @pl.when(jnp.logical_not(own))
            def _():
                recv[b, part(sub), :] = res

            return 0

        lax.fori_loop(lo, hi, one, 0)

    def combine(g, mb, width=2 * cap):
        for hi in range(width // cap):
            i = g * 4 + (1 - hi) * 2 + mb

            @pl.when(jnp.logical_not(home_own(i)))
            def _():
                ret_arrival(i).wait_recv()

        want = lax.broadcasted_iota(jnp.int32, (LANES, width), 1).astype(F32) + (g * 2 * cap).astype(F32)
        size = c_buf.shape[0]
        for blk in range(tok // size):
            for s in range(size // LANES):
                n = blk * (size // LANES) + s
                c_buf[s * LANES:(s + 1) * LANES, 0:width] = jnp.where(col_buf[mb, :, n:n + 1] == want, 1.0, 0.0).astype(BF16)
            picked = dot(c_buf[:, 0:width], back[g, mb, 0:width, :])
            for s in range(size // LANES):
                n = blk * (size // LANES) + s
                at = slice(n * LANES, (n + 1) * LANES)
                gate = col_buf[mb, :, groups + n:groups + n + 1]
                xbuf[mb, at, :] = (xbuf[mb, at, :].astype(F32) + gate * picked[s * LANES:(s + 1) * LANES, :]).astype(BF16)

    @pl.when(is_a)
    def _():
        pl.semaphore_wait(go, 1)
        lax.fori_loop(0, nf, start_remote, 0)

        def expert(j, _):
            lo, hi = j * 4, j * 4 + 4
            lax.fori_loop(lo, hi, clear, 0)
            lax.fori_loop(lo, hi, wait_tokens, 0)

            def refill(k):
                @pl.when(j == 0)
                def _():
                    pl.semaphore_signal(credit, inc=1, device_id=y_other)
                    pl.semaphore_wait(credit, 1)
                    for c in w_remote(1, k) + w_local(1, k):
                        c.start()

            def chunk(k, _):
                wait_weights(k)
                add_chunk(k, j * 2, j * 2 + 2)
                refill(k)

                return 0

            lax.fori_loop(0, nf - 1, chunk, 0)
            last_parts = list(zip(w_local(0, nf - 1), w_remote(0, nf - 1)))
            for n, (local, remote) in enumerate(last_parts):
                local.wait()
                remote.wait()
                if n == SIGNAL_AFTER:
                    @pl.when(j == 1)
                    def _():
                        pl.semaphore_signal(go, inc=1, device_id=device(0, 0, 1))

            finish(lo * 2, lo * 2, hi * 2, (nf - 1,))
            ret_copy(hi - 1, 1).start()
            refill(nf - 1)
            return 0

        lax.fori_loop(0, 2, expert, 0)

    def combine_both(g):
        def step(mb, _):
            combine(g, mb)
            return 0

        lax.fori_loop(0, n_mb, step, 0)

    @pl.when(is_b)
    def _():
        for c in w_remote(j_out, early - 3):
            c.wait_send()
        pl.semaphore_signal(go, inc=1, device_id=device(0, 0, 0))
        lax.fori_loop(0, 8, clear, 0)
        lax.fori_loop(0, 8, wait_tokens, 0)

        def chunk(k, _):
            for c in w_local(0, k):
                c.wait()
            for c in w_remote(0, k):
                c.wait_recv()

            @pl.when(k != early - 3)
            def _():
                for c in w_remote(0, k):
                    c.wait_send()

            @pl.when(k < nf - 1)
            def _():
                add_chunk(k, 0, jnp.where(k == nf - 2, 3, 4))

            @pl.when(k == early - 1)
            def _():
                combine_both(jnp.int32(2))
                pl.semaphore_wait(go, 1)
                lax.fori_loop(early, nf, start_remote, 0)

            return 0

        lax.fori_loop(0, nf, chunk, 0)
        finish(0, 0, 4, (nf - 1,))
        finish(0, 4, 8, (nf - 2, nf - 1))
        finish(0, 8, 16, (nf - 1,))

    def late(n, _):
        pair = lax.div(n, 2)
        g = jnp.where(pair < 2, pair + 2, 3 - pair)
        combine(g, lax.rem(n, 2))
        return 0

    lax.fori_loop(2 * c_me, 6, late, 0)
    outs = [pltpu.make_async_copy(xbuf.at[mb], y_hbm.at[mb], y_sem.at[mb]) for mb in range(n_mb)]
    col_out = pltpu.make_async_copy(col_buf.at[1], col_hbm, col_sem)
    combine(jnp.int32(0), jnp.int32(1), cap)
    outs[1].start()
    col_out.start()
    combine(jnp.int32(0), jnp.int32(0))
    outs[0].start()
    pltpu.make_async_remote_copy(send.at[0], tail_hbm, ret_send.at[0], ret_recv.at[1],
                                 device_id=device(1, 0, 0)).wait_recv()

    def drain(i, _):
        @pl.when(jnp.logical_not(home_own(i)))
        def _():
            tok_copy(i).wait_send()

        b, sub = lax.div(i, 2), lax.rem(i, 2)

        @pl.when(jnp.logical_not(slot_own(b, sub)))
        def _():
            ret_do(b, sub, lambda c: c.wait_send())

        return 0

    lax.fori_loop(0, 16, drain, 0)
    for c in outs + [col_out]:
        c.wait()


def tail_kernel(cap, y_hbm, col_hbm, tail_hbm, out_hbm, buf, col, tail, c_buf, in_sem, out_sem, col_sem, tail_sem):
    n_mb, tok, _ = buf.shape
    parts = 4
    size = tok // parts
    per = size // LANES
    groups = tok // LANES
    loads = [pltpu.make_async_copy(col_hbm, col, col_sem), pltpu.make_async_copy(tail_hbm, tail, tail_sem)]
    for c in loads:
        c.start()

    def rows_at(p):
        return p // parts, pl.ds((p % parts) * size, size)

    def move(p, out):
        mb, at = rows_at(p)
        if out:
            return pltpu.make_async_copy(buf.at[mb, at, :], out_hbm.at[mb, at, :], out_sem.at[p])
        return pltpu.make_async_copy(y_hbm.at[mb, at, :], buf.at[mb, at, :], in_sem.at[p])

    for p in range(n_mb * parts):
        move(p, False).start()
    loads[0].wait()
    want = lax.broadcasted_iota(jnp.int32, (LANES, cap), 1).astype(F32) + float(cap)
    for n in range(groups):
        c_buf[n * LANES:(n + 1) * LANES, :] = jnp.where(col[:, n:n + 1] == want, 1.0, 0.0).astype(BF16)
    loads[1].wait()
    for p in range(parts):
        move(p, False).wait()
        move(p, True).start()
    for p in range(parts, 2 * parts):
        blk = p - parts
        picked = dot(c_buf[blk * size:(blk + 1) * size, :], tail[...])
        move(p, False).wait()
        for s in range(per):
            n = blk * per + s
            at = slice(n * LANES, (n + 1) * LANES)
            gate = col[:, groups + n:groups + n + 1]
            part = picked[s * LANES:(s + 1) * LANES, :]
            buf[1, at, :] = (buf[1, at, :].astype(F32) + gate * part).astype(BF16)
        move(p, True).start()
    for p in range(2 * parts):
        move(p, True).wait()


def solution(mesh):
    row_spec = P(None, ('rep', 'expert', 'data'), None)
    up_spec = P('expert', 'data', None)
    down_spec = P('expert', None, 'data')

    def per_device(x_loc, idx_loc, gate_loc, wg_loc, wu_loc, wd_loc):
        n_mb, tok, d_model = x_loc.shape
        n_loc, half, ff = wg_loc.shape
        n_exp = n_loc * mesh.shape['expert']
        n_top = idx_loc.shape[2]
        assert n_top == 1 and n_exp == 8 and n_mb == 2
        cap = 8 * ((5 * n_top * tok + 32 * n_exp - 1) // (32 * n_exp))
        fc = 256
        nf = ff // fc
        early = 8
        groups = tok // LANES
        hbm = pl.BlockSpec(memory_space=pl.ANY)
        vmem = pl.BlockSpec(memory_space=pltpu.VMEM)
        dma = pltpu.SemaphoreType.DMA
        y_part, col, tail = pl.pallas_call(
            functools.partial(moe_kernel, (cap, fc, nf, early)),
            out_shape=(jax.ShapeDtypeStruct(x_loc.shape, BF16), jax.ShapeDtypeStruct((LANES, LANES), F32),
                       jax.ShapeDtypeStruct((cap, d_model), BF16)),
            in_specs=[vmem, vmem, hbm, hbm, hbm, hbm],
            out_specs=(hbm, hbm, hbm),
            scratch_shapes=[
                pltpu.VMEM((n_mb, tok, d_model), BF16),
                pltpu.VMEM((14, cap, d_model), BF16),
                pltpu.VMEM((8, 2 * cap, d_model), BF16),
                pltpu.VMEM((4, n_mb, 2 * cap, d_model), BF16),
                pltpu.VMEM((8, 2 * cap, d_model), F32),
                pltpu.VMEM((nf, d_model, fc), BF16),
                pltpu.VMEM((nf, d_model, fc), BF16),
                pltpu.VMEM((nf, fc, d_model), BF16),
                pltpu.VMEM((cap, tok // 2), BF16),
                pltpu.VMEM((512, 2 * cap), BF16),
                pltpu.VMEM((n_mb, groups, LANES), F32),
                pltpu.VMEM((n_mb, LANES, LANES), F32),
                pltpu.VMEM((n_mb, LANES, LANES), F32),
                dma((n_mb,)), dma((n_mb,)), dma,
                dma((16,)), dma((16,)), dma((16,)), dma((16,)),
                dma((nf, 3)), dma((nf, 3)), dma((nf, 3)),
                pltpu.SemaphoreType.REGULAR, pltpu.SemaphoreType.REGULAR,
            ],
            compiler_params=pltpu.CompilerParams(
                collective_id=0, has_side_effects=True, vmem_limit_bytes=64 * 1024 * 1024 - 65536),
        )(idx_loc.reshape(n_mb, groups, LANES), gate_loc.reshape(n_mb, groups, LANES), x_loc, wg_loc, wu_loc, wd_loc)
        return pl.pallas_call(
            functools.partial(tail_kernel, cap),
            out_shape=jax.ShapeDtypeStruct(x_loc.shape, BF16),
            in_specs=[hbm, hbm, hbm],
            out_specs=hbm,
            scratch_shapes=[
                pltpu.VMEM((n_mb, tok, d_model), BF16), pltpu.VMEM((LANES, LANES), F32), pltpu.VMEM((cap, d_model), BF16),
                pltpu.VMEM((tok, cap), BF16), dma((8,)), dma((8,)), dma, dma,
            ],
        )(y_part, col, tail)

    return jax.shard_map(per_device, mesh=mesh, in_specs=(row_spec, row_spec, row_spec, up_spec, up_spec, down_spec),
                         out_specs=row_spec, check_vma=False)
```

```python
import functools

import jax
import jax.numpy as jnp
from jax import lax
from jax.experimental import pallas as pl
from jax.experimental.pallas import tpu as pltpu
from jax.sharding import PartitionSpec as P

F32 = jnp.float32
BF16 = jnp.bfloat16
LANES = 128
SIGNAL_AFTER = 1


def dot(a, b):
    return jnp.dot(a, b, preferred_element_type=F32)


def moe_kernel(dims, ids_hbm, gate_hbm, x_hbm, wg_hbm, wu_hbm, wd_hbm, y_hbm, col_hbm, tail_hbm,
               ids_ref, gate_ref, h_buf, xbuf, send, recv, back, oacc, wg_buf, wu_buf, wd_buf, p_buf, c_buf, slot_buf, cat_buf, col_buf,
               in_sem, x_sem, y_sem, col_sem, tok_send, tok_recv, ret_send, ret_recv, w_send, w_recv, w_loc, credit, go):
    cap, fc, nf, early = dims
    n_mb, tok, d_model = xbuf.shape
    half = d_model // 2
    groups = tok // LANES
    q_me = lax.axis_index('expert')
    y_me = lax.axis_index('data')
    x_me, c_me = lax.div(q_me, 2), lax.rem(q_me, 2)
    is_a = c_me == 0
    is_b = c_me == 1

    def device(dx, dy, c):
        return {'expert': lax.rem(x_me + dx, 2) * 2 + c, 'data': lax.rem(y_me + dy, 2)}

    def piece(i):
        g = lax.div(i, 4)
        hi = 1 - lax.div(lax.rem(i, 4), 2)
        return g, hi, lax.rem(i, 2)

    def home_own(i):
        g, hi, _ = piece(i)
        return (hi == 0) & (((g >= 2) & is_a) | ((g == 1) & is_b))

    def slot_own(b, sub):
        hi = 1 - lax.div(lax.rem(b, 4), 2)
        return (hi == 0) & (sub == c_me) & (is_a | (b >= 4))

    def part(sub):
        return pl.ds(pl.multiple_of(sub * cap, cap), cap)

    def send_at(i):
        return jnp.where(i < 10, i, jnp.where(i < 12, i - 4, i - 2))

    def tok_copy(i):
        g, hi, mb = piece(i)
        dev = device(hi, jnp.where(g == 0, 1, 0), jnp.where(g >= 2, 0, 1))
        b = lax.rem(i, 8)
        return pltpu.make_async_remote_copy(send.at[send_at(i)], recv.at[b, part(c_me), :], tok_send.at[i],
                                            tok_recv.at[b * 2 + c_me], device_id=dev)

    def tok_arrival(b, sub):
        return pltpu.make_async_remote_copy(send.at[0], recv.at[b, part(sub), :], tok_send.at[0],
                                            tok_recv.at[b * 2 + sub], device_id=device(1, 0, 0))

    def ret_copy(b, sub, tail=False):
        g = (1 - c_me) * 2 + lax.div(b, 4)
        hi = 1 - lax.div(lax.rem(b, 4), 2)
        mb = lax.rem(b, 2)
        dev = device(hi, jnp.where(g == 0, 1, 0), sub)
        i = (1 - c_me) * 8 + b
        dst = tail_hbm if tail else back.at[g, mb, part(hi), :]
        return pltpu.make_async_remote_copy(recv.at[b, part(sub), :], dst,
                                            ret_send.at[b * 2 + sub], ret_recv.at[i], device_id=dev)

    def ret_do(b, sub, what):
        tail = is_b & (b == 1)

        @pl.when(tail)
        def _():
            what(ret_copy(b, sub, True))

        @pl.when(jnp.logical_not(tail))
        def _():
            what(ret_copy(b, sub))

    def ret_arrival(i):
        g, hi, mb = piece(i)
        return pltpu.make_async_remote_copy(send.at[0], back.at[g, mb, part(hi), :], ret_send.at[0],
                                            ret_recv.at[i], device_id=device(1, 0, 0))

    y_other = {'data': 1 - y_me}
    my_half = pl.ds(pl.multiple_of(y_me * half, half), half)

    def w_parts(j, k):
        cols = pl.ds(pl.multiple_of(k * fc, fc), fc)
        return ((wg_hbm.at[j, :, cols], wg_buf.at[k, my_half, :], 0),
                (wu_hbm.at[j, :, cols], wu_buf.at[k, my_half, :], 1),
                (wd_hbm.at[j, cols, :], wd_buf.at[k, :, my_half], 2))

    def w_remote(j, k):
        return [pltpu.make_async_remote_copy(s, d, w_send.at[k, n], w_recv.at[k, n], device_id=y_other)
                for s, d, n in w_parts(j, k)]

    def w_local(j, k):
        return [pltpu.make_async_copy(s, d, w_loc.at[k, n]) for s, d, n in w_parts(j, k)]

    barrier = pltpu.get_barrier_semaphore()
    for n in range(1, 8):
        other = device(n // 4, (n // 2) % 2, lax.rem(c_me + n % 2, 2))
        pl.semaphore_signal(barrier, inc=1, device_id=other)
    pl.semaphore_wait(barrier, 7)

    j_out = jnp.where(is_a, 0, 1 - y_me)
    j_in = jnp.where(is_a, 0, y_me)

    def start_remote(k, _):
        for c in w_remote(j_out, k):
            c.start()
        return 0

    def start_local(k, _):
        for c in w_local(j_in, k):
            c.start()
        return 0

    lax.fori_loop(0, early * c_me, start_remote, 0)
    small = [pltpu.make_async_copy(ids_hbm, ids_ref, in_sem.at[0]), pltpu.make_async_copy(gate_hbm, gate_ref, in_sem.at[1])]
    for c in small:
        c.start()
    x_loads = [pltpu.make_async_copy(x_hbm.at[mb], xbuf.at[mb], x_sem.at[mb]) for mb in range(n_mb)]
    for c in x_loads:
        c.start()
    lax.fori_loop(0, nf, start_local, 0)

    for c in small:
        c.wait()
    masks = []
    for mb in range(n_mb):
        ids = ids_ref[mb]
        for e in range(8):
            masks.append((ids == e).astype(F32))
    stack = jnp.concatenate(masks, axis=0).astype(BF16)
    rows = stack.shape[0]
    lane_r = lax.broadcasted_iota(jnp.int32, (LANES, LANES), 0)
    lane_c = lax.broadcasted_iota(jnp.int32, (LANES, LANES), 1)
    upper = jnp.where(lane_r < lane_c, 1.0, 0.0).astype(BF16)
    row_r = lax.broadcasted_iota(jnp.int32, (rows, rows), 0)
    row_c = lax.broadcasted_iota(jnp.int32, (rows, rows), 1)
    first = row_r - lax.rem(row_r, groups)
    lower = jnp.where((row_c >= first) & (row_c < row_r), 1.0, 0.0).astype(BF16)
    ones = jnp.ones((LANES, LANES), BF16)
    prefix = dot(stack, upper) + dot(dot(lower, stack).astype(BF16), ones)
    cat_buf[...] = jnp.zeros_like(cat_buf)
    for mb in range(n_mb):
        place = jnp.full((groups, LANES), -1.0, F32)
        for e in range(8):
            r0 = (mb * 8 + e) * groups
            slot = prefix[r0:r0 + groups]
            x_e, c_e, j = e // 4, (e // 2) % 2, e % 2
            hi = lax.rem(x_me + x_e, 2)
            g = 1 - lax.rem(y_me + j, 2) if c_e else 2 + j
            base = ((g * 2 + hi) * cap).astype(F32)
            place = jnp.where((masks[mb * 8 + e] > 0.5) & (slot < float(cap)), base + slot, place)
        slot_buf[mb] = place
        cat_buf[mb, 0:groups, :] = place
        cat_buf[mb, groups:2 * groups, :] = gate_ref[mb]
        col_buf[mb] = cat_buf[mb].T

    for c in x_loads:
        c.wait()

    def dispatch(i, _):
        g, hi, mb = piece(i)
        base = ((g * 2 + hi) * cap).astype(F32)
        want = lax.broadcasted_iota(jnp.int32, (cap, LANES), 0).astype(F32) + base
        place = slot_buf[mb]
        out = None
        for h in range(2):
            for n in range(groups // 2):
                at = h * (groups // 2) + n
                p_buf[:, n * LANES:(n + 1) * LANES] = jnp.where(place[at:at + 1, :] == want, 1.0, 0.0).astype(BF16)
            picked = dot(p_buf[...], xbuf[mb, h * (tok // 2):(h + 1) * (tok // 2), :])
            out = picked if h == 0 else (out + picked).astype(BF16)
        own = home_own(i)

        @pl.when(own)
        def _():
            recv[lax.rem(i, 8), part(c_me), :] = out

        @pl.when(jnp.logical_not(own))
        def _():
            send[send_at(i)] = out

        @pl.when((i > 0) & jnp.logical_not(home_own(i - 1)))
        def _():
            tok_copy(i - 1).start()

        return 0

    lax.fori_loop(0, 16, dispatch, 0)

    @pl.when(is_b)
    def _():
        tok_copy(15).start()

    def wait_tokens(b, _):
        for sub in range(2):
            @pl.when(jnp.logical_not(slot_own(b, sub)))
            def _():
                tok_arrival(b, sub).wait_recv()
        return 0

    def wait_weights(k):
        for local, remote in zip(w_local(0, k), w_remote(0, k)):
            local.wait()
            remote.wait()

    def pre(rows_in, k):
        return dot(rows_in, wg_buf[k]), dot(rows_in, wu_buf[k])

    def hidden(gate_up):
        gate_pre, up_pre = gate_up
        return (gate_pre / (1.0 + jnp.exp(-gate_pre)) * up_pre).astype(BF16)

    def post(gate_up, k):
        return dot(hidden(gate_up), wd_buf[k])

    def clear(b, _):
        oacc[b] = jnp.zeros_like(oacc[b])
        return 0

    def add_chunk(k, lo, hi):
        def pair(p, _):
            one = jnp.where(is_a, p * 2, jnp.where(p < 2, p * 6, p))
            two = jnp.where(is_a | (p < 2), one + 1, p + 2)
            both = [(b, pre(recv[b], k)) for b in (one, two)]
            for b, pre_b in both:
                oacc[b] += post(pre_b, k)
            return 0

        lax.fori_loop(lo, hi, pair, 0)

    def slot_of(r):
        t = lax.div(r, 2)
        straight = 2 + lax.rem(t, 2) * 2 + lax.div(t, 2)
        return jnp.where(is_a | (t >= 6), t, jnp.where(t < 4, straight, t - 4)), lax.rem(r, 2)

    def finish(start, lo, hi, chunks, ready=False):
        def one(r, _):
            b_old, sub_old = slot_of(r - 1)

            @pl.when((r > start) & jnp.logical_not(slot_own(b_old, sub_old)))
            def _():
                ret_do(b_old, sub_old, lambda c: c.start())

            b, sub = slot_of(r)
            rows_in = recv[b, part(sub), :]
            total = oacc[b, part(sub), :]
            if ready:
                total = total + dot(h_buf[part(sub), :], wd_buf[nf - 1])
            for k in chunks:
                total = total + post(pre(rows_in, k), k)
            res = total.astype(BF16)
            own = slot_own(b, sub)

            @pl.when(own)
            def _():
                back[(1 - c_me) * 2 + lax.div(b, 4), lax.rem(b, 2), 0:cap, :] = res

            @pl.when(jnp.logical_not(own))
            def _():
                recv[b, part(sub), :] = res

            return 0

        lax.fori_loop(lo, hi, one, 0)

    def combine(g, mb, width=2 * cap):
        for hi in range(width // cap):
            i = g * 4 + (1 - hi) * 2 + mb

            @pl.when(jnp.logical_not(home_own(i)))
            def _():
                ret_arrival(i).wait_recv()

        want = lax.broadcasted_iota(jnp.int32, (LANES, width), 1).astype(F32) + (g * 2 * cap).astype(F32)
        size = c_buf.shape[0]
        for blk in range(tok // size):
            for s in range(size // LANES):
                n = blk * (size // LANES) + s
                c_buf[s * LANES:(s + 1) * LANES, 0:width] = jnp.where(col_buf[mb, :, n:n + 1] == want, 1.0, 0.0).astype(BF16)
            picked = dot(c_buf[:, 0:width], back[g, mb, 0:width, :])
            for s in range(size // LANES):
                n = blk * (size // LANES) + s
                at = slice(n * LANES, (n + 1) * LANES)
                gate = col_buf[mb, :, groups + n:groups + n + 1]
                xbuf[mb, at, :] = (xbuf[mb, at, :].astype(F32) + gate * picked[s * LANES:(s + 1) * LANES, :]).astype(BF16)

    @pl.when(is_a)
    def _():
        pl.semaphore_wait(go, 1)
        lax.fori_loop(0, nf, start_remote, 0)

        def expert(j, _):
            lo, hi = j * 4, j * 4 + 4
            lax.fori_loop(lo, hi, clear, 0)
            lax.fori_loop(lo, hi, wait_tokens, 0)

            def refill(k):
                @pl.when(j == 0)
                def _():
                    pl.semaphore_signal(credit, inc=1, device_id=y_other)
                    pl.semaphore_wait(credit, 1)
                    for c in w_remote(1, k) + w_local(1, k):
                        c.start()

            def chunk(k, _):
                wait_weights(k)
                add_chunk(k, j * 2, j * 2 + 2)
                refill(k)

                return 0

            lax.fori_loop(0, nf - 1, chunk, 0)
            last_parts = list(zip(w_local(0, nf - 1), w_remote(0, nf - 1)))
            for n, (local, remote) in enumerate(last_parts):
                local.wait()
                remote.wait()
                if n == SIGNAL_AFTER:
                    @pl.when(j == 1)
                    def _():
                        pl.semaphore_signal(go, inc=1, device_id=device(0, 0, 1))

            finish(lo * 2, lo * 2, hi * 2, (nf - 1,))
            ret_copy(hi - 1, 1).start()
            refill(nf - 1)
            return 0

        lax.fori_loop(0, 2, expert, 0)

    def combine_both(g):
        def step(mb, _):
            combine(g, mb)
            return 0

        lax.fori_loop(0, n_mb, step, 0)

    @pl.when(is_b)
    def _():
        for c in w_remote(j_out, early - 3):
            c.wait_send()
        pl.semaphore_signal(go, inc=1, device_id=device(0, 0, 0))
        lax.fori_loop(0, 8, clear, 0)
        lax.fori_loop(0, 8, wait_tokens, 0)

        def chunk(k, _):
            for c in w_local(0, k):
                c.wait()
            for c in w_remote(0, k):
                c.wait_recv()

            @pl.when(k != early - 3)
            def _():
                for c in w_remote(0, k):
                    c.wait_send()

            add_chunk(k, 0, jnp.where(k == nf - 2, 3, 4))

            @pl.when(k == early - 1)
            def _():
                combine_both(jnp.int32(2))
                pl.semaphore_wait(go, 1)
                lax.fori_loop(early, nf, start_remote, 0)

            return 0

        lax.fori_loop(0, nf - 1, chunk, 0)
        for n, (local, remote) in enumerate(zip(w_local(0, nf - 1), w_remote(0, nf - 1))):
            local.wait()
            remote.wait()
            if n == 1:
                h_buf[...] = hidden(pre(recv[2], nf - 1))
        finish(0, 0, 2, (), ready=True)
        finish(0, 2, 4, (nf - 1,))
        finish(0, 4, 8, (nf - 2, nf - 1))
        finish(0, 8, 16, (nf - 1,))

    def late(n, _):
        pair = lax.div(n, 2)
        g = jnp.where(pair < 2, pair + 2, 3 - pair)
        combine(g, lax.rem(n, 2))
        return 0

    lax.fori_loop(2 * c_me, 6, late, 0)
    outs = [pltpu.make_async_copy(xbuf.at[mb], y_hbm.at[mb], y_sem.at[mb]) for mb in range(n_mb)]
    col_out = pltpu.make_async_copy(col_buf.at[1], col_hbm, col_sem)
    combine(jnp.int32(0), jnp.int32(1), cap)
    outs[1].start()
    col_out.start()
    combine(jnp.int32(0), jnp.int32(0))
    outs[0].start()
    pltpu.make_async_remote_copy(send.at[0], tail_hbm, ret_send.at[0], ret_recv.at[1],
                                 device_id=device(1, 0, 0)).wait_recv()

    def drain(i, _):
        @pl.when(jnp.logical_not(home_own(i)))
        def _():
            tok_copy(i).wait_send()

        b, sub = lax.div(i, 2), lax.rem(i, 2)

        @pl.when(jnp.logical_not(slot_own(b, sub)))
        def _():
            ret_do(b, sub, lambda c: c.wait_send())

        return 0

    lax.fori_loop(0, 16, drain, 0)
    for c in outs + [col_out]:
        c.wait()


def tail_kernel(cap, y_hbm, col_hbm, tail_hbm, out_hbm, buf, col, tail, c_buf, in_sem, out_sem, col_sem, tail_sem):
    n_mb, tok, _ = buf.shape
    parts = 4
    size = tok // parts
    per = size // LANES
    groups = tok // LANES
    loads = [pltpu.make_async_copy(col_hbm, col, col_sem), pltpu.make_async_copy(tail_hbm, tail, tail_sem)]
    for c in loads:
        c.start()

    def rows_at(p):
        return p // parts, pl.ds((p % parts) * size, size)

    def move(p, out):
        mb, at = rows_at(p)
        if out:
            return pltpu.make_async_copy(buf.at[mb, at, :], out_hbm.at[mb, at, :], out_sem.at[p])
        return pltpu.make_async_copy(y_hbm.at[mb, at, :], buf.at[mb, at, :], in_sem.at[p])

    for p in range(n_mb * parts):
        move(p, False).start()
    loads[0].wait()
    want = lax.broadcasted_iota(jnp.int32, (LANES, cap), 1).astype(F32) + float(cap)
    for n in range(groups):
        c_buf[n * LANES:(n + 1) * LANES, :] = jnp.where(col[:, n:n + 1] == want, 1.0, 0.0).astype(BF16)
    loads[1].wait()
    for p in range(parts):
        move(p, False).wait()
        move(p, True).start()
    for p in range(parts, 2 * parts):
        blk = p - parts
        picked = dot(c_buf[blk * size:(blk + 1) * size, :], tail[...])
        move(p, False).wait()
        for s in range(per):
            n = blk * per + s
            at = slice(n * LANES, (n + 1) * LANES)
            gate = col[:, groups + n:groups + n + 1]
            part = picked[s * LANES:(s + 1) * LANES, :]
            buf[1, at, :] = (buf[1, at, :].astype(F32) + gate * part).astype(BF16)
        move(p, True).start()
    for p in range(2 * parts):
        move(p, True).wait()


def solution(mesh):
    row_spec = P(None, ('rep', 'expert', 'data'), None)
    up_spec = P('expert', 'data', None)
    down_spec = P('expert', None, 'data')

    def per_device(x_loc, idx_loc, gate_loc, wg_loc, wu_loc, wd_loc):
        n_mb, tok, d_model = x_loc.shape
        n_loc, half, ff = wg_loc.shape
        n_exp = n_loc * mesh.shape['expert']
        n_top = idx_loc.shape[2]
        assert n_top == 1 and n_exp == 8 and n_mb == 2
        cap = 8 * ((5 * n_top * tok + 32 * n_exp - 1) // (32 * n_exp))
        fc = 256
        nf = ff // fc
        early = 8
        groups = tok // LANES
        hbm = pl.BlockSpec(memory_space=pl.ANY)
        dma = pltpu.SemaphoreType.DMA
        y_part, col, tail = pl.pallas_call(
            functools.partial(moe_kernel, (cap, fc, nf, early)),
            out_shape=(jax.ShapeDtypeStruct(x_loc.shape, BF16), jax.ShapeDtypeStruct((LANES, LANES), F32),
                       jax.ShapeDtypeStruct((cap, d_model), BF16)),
            in_specs=[hbm] * 6,
            out_specs=(hbm, hbm, hbm),
            scratch_shapes=[
                pltpu.VMEM((n_mb, groups, LANES), jnp.int32), pltpu.VMEM((n_mb, groups, LANES), F32),
                pltpu.VMEM((2 * cap, fc), BF16),
                pltpu.VMEM((n_mb, tok, d_model), BF16),
                pltpu.VMEM((14, cap, d_model), BF16),
                pltpu.VMEM((8, 2 * cap, d_model), BF16),
                pltpu.VMEM((4, n_mb, 2 * cap, d_model), BF16),
                pltpu.VMEM((8, 2 * cap, d_model), F32),
                pltpu.VMEM((nf, d_model, fc), BF16),
                pltpu.VMEM((nf, d_model, fc), BF16),
                pltpu.VMEM((nf, fc, d_model), BF16),
                pltpu.VMEM((cap, tok // 2), BF16),
                pltpu.VMEM((512, 2 * cap), BF16),
                pltpu.VMEM((n_mb, groups, LANES), F32),
                pltpu.VMEM((n_mb, LANES, LANES), F32),
                pltpu.VMEM((n_mb, LANES, LANES), F32),
                dma((2,)), dma((n_mb,)), dma((n_mb,)), dma,
                dma((16,)), dma((16,)), dma((16,)), dma((16,)),
                dma((nf, 3)), dma((nf, 3)), dma((nf, 3)),
                pltpu.SemaphoreType.REGULAR, pltpu.SemaphoreType.REGULAR,
            ],
            compiler_params=pltpu.CompilerParams(
                collective_id=0, has_side_effects=True, vmem_limit_bytes=64 * 1024 * 1024 - 65536),
        )(idx_loc.reshape(n_mb, groups, LANES), gate_loc.reshape(n_mb, groups, LANES), x_loc, wg_loc, wu_loc, wd_loc)
        return pl.pallas_call(
            functools.partial(tail_kernel, cap),
            out_shape=jax.ShapeDtypeStruct(x_loc.shape, BF16),
            in_specs=[hbm, hbm, hbm],
            out_specs=hbm,
            scratch_shapes=[
                pltpu.VMEM((n_mb, tok, d_model), BF16), pltpu.VMEM((LANES, LANES), F32), pltpu.VMEM((cap, d_model), BF16),
                pltpu.VMEM((tok, cap), BF16), dma((8,)), dma((8,)), dma, dma,
            ],
        )(y_part, col, tail)

    return jax.shard_map(per_device, mesh=mesh, in_specs=(row_spec, row_spec, row_spec, up_spec, up_spec, down_spec),
                         out_specs=row_spec, check_vma=False)
```

```python
import functools

import jax
import jax.numpy as jnp
from jax import lax
from jax.experimental import pallas as pl
from jax.experimental.pallas import tpu as pltpu
from jax.sharding import PartitionSpec as P

F32 = jnp.float32
BF16 = jnp.bfloat16
LANES = 128
SIGNAL_AFTER = 1


def dot(a, b):
    return jnp.dot(a, b, preferred_element_type=F32)


def moe_kernel(dims, ids_hbm, gate_hbm, x_hbm, wg_hbm, wu_hbm, wd_hbm, y_hbm, col_hbm, tail_hbm,
               ids_ref, gate_ref, h_buf, xbuf, send, recv, back, oacc, wg_buf, wu_buf, wd_buf, p_buf, c_buf, slot_buf, cat_buf, col_buf,
               in_sem, x_sem, y_sem, col_sem, tok_send, tok_recv, ret_send, ret_recv, w_send, w_recv, w_loc, credit, go):
    cap, fc, nf, early = dims
    n_mb, tok, d_model = xbuf.shape
    half = d_model // 2
    groups = tok // LANES
    q_me = lax.axis_index('expert')
    y_me = lax.axis_index('data')
    x_me, c_me = lax.div(q_me, 2), lax.rem(q_me, 2)
    is_a = c_me == 0
    is_b = c_me == 1

    def device(dx, dy, c):
        return {'expert': lax.rem(x_me + dx, 2) * 2 + c, 'data': lax.rem(y_me + dy, 2)}

    def piece(i):
        g = lax.div(i, 4)
        hi = 1 - lax.div(lax.rem(i, 4), 2)
        return g, hi, lax.rem(i, 2)

    def home_own(i):
        g, hi, _ = piece(i)
        return (hi == 0) & (((g >= 2) & is_a) | ((g == 1) & is_b))

    def slot_own(b, sub):
        hi = 1 - lax.div(lax.rem(b, 4), 2)
        return (hi == 0) & (sub == c_me) & (is_a | (b >= 4))

    def part(sub):
        return pl.ds(pl.multiple_of(sub * cap, cap), cap)

    def send_at(i):
        return jnp.where(i < 10, i, jnp.where(i < 12, i - 4, i - 2))

    def tok_copy(i):
        g, hi, mb = piece(i)
        dev = device(hi, jnp.where(g == 0, 1, 0), jnp.where(g >= 2, 0, 1))
        b = lax.rem(i, 8)
        return pltpu.make_async_remote_copy(send.at[send_at(i)], recv.at[b, part(c_me), :], tok_send.at[i],
                                            tok_recv.at[b * 2 + c_me], device_id=dev)

    def tok_arrival(b, sub):
        return pltpu.make_async_remote_copy(send.at[0], recv.at[b, part(sub), :], tok_send.at[0],
                                            tok_recv.at[b * 2 + sub], device_id=device(1, 0, 0))

    def ret_copy(b, sub, tail=False):
        g = (1 - c_me) * 2 + lax.div(b, 4)
        hi = 1 - lax.div(lax.rem(b, 4), 2)
        mb = lax.rem(b, 2)
        dev = device(hi, jnp.where(g == 0, 1, 0), sub)
        i = (1 - c_me) * 8 + b
        dst = tail_hbm if tail else back.at[g, mb, part(hi), :]
        return pltpu.make_async_remote_copy(recv.at[b, part(sub), :], dst,
                                            ret_send.at[b * 2 + sub], ret_recv.at[i], device_id=dev)

    def ret_do(b, sub, what):
        tail = is_b & (b == 1)

        @pl.when(tail)
        def _():
            what(ret_copy(b, sub, True))

        @pl.when(jnp.logical_not(tail))
        def _():
            what(ret_copy(b, sub))

    def ret_arrival(i):
        g, hi, mb = piece(i)
        return pltpu.make_async_remote_copy(send.at[0], back.at[g, mb, part(hi), :], ret_send.at[0],
                                            ret_recv.at[i], device_id=device(1, 0, 0))

    y_other = {'data': 1 - y_me}
    my_half = pl.ds(pl.multiple_of(y_me * half, half), half)

    def w_parts(j, k):
        cols = pl.ds(pl.multiple_of(k * fc, fc), fc)
        return ((wg_hbm.at[j, :, cols], wg_buf.at[k, my_half, :], 0),
                (wu_hbm.at[j, :, cols], wu_buf.at[k, my_half, :], 1),
                (wd_hbm.at[j, cols, :], wd_buf.at[k, :, my_half], 2))

    def w_remote(j, k):
        return [pltpu.make_async_remote_copy(s, d, w_send.at[k, n], w_recv.at[k, n], device_id=y_other)
                for s, d, n in w_parts(j, k)]

    def w_local(j, k):
        return [pltpu.make_async_copy(s, d, w_loc.at[k, n]) for s, d, n in w_parts(j, k)]

    barrier = pltpu.get_barrier_semaphore()
    for n in range(1, 8):
        other = device(n // 4, (n // 2) % 2, lax.rem(c_me + n % 2, 2))
        pl.semaphore_signal(barrier, inc=1, device_id=other)
    pl.semaphore_wait(barrier, 7)

    j_out = jnp.where(is_a, 0, 1 - y_me)
    j_in = jnp.where(is_a, 0, y_me)

    def start_remote(k, _):
        for c in w_remote(j_out, k):
            c.start()
        return 0

    def start_local(k, _):
        for c in w_local(j_in, k):
            c.start()
        return 0

    lax.fori_loop(0, early * c_me, start_remote, 0)
    small = [pltpu.make_async_copy(ids_hbm, ids_ref, in_sem.at[0]), pltpu.make_async_copy(gate_hbm, gate_ref, in_sem.at[1])]
    for c in small:
        c.start()
    x_loads = [pltpu.make_async_copy(x_hbm.at[mb], xbuf.at[mb], x_sem.at[mb]) for mb in range(n_mb)]
    for c in x_loads:
        c.start()
    lax.fori_loop(0, nf, start_local, 0)

    for c in small:
        c.wait()
    masks = []
    for mb in range(n_mb):
        ids = ids_ref[mb]
        for e in range(8):
            masks.append((ids == e).astype(F32))
    stack = jnp.concatenate(masks, axis=0).astype(BF16)
    rows = stack.shape[0]
    lane_r = lax.broadcasted_iota(jnp.int32, (LANES, LANES), 0)
    lane_c = lax.broadcasted_iota(jnp.int32, (LANES, LANES), 1)
    upper = jnp.where(lane_r < lane_c, 1.0, 0.0).astype(BF16)
    row_r = lax.broadcasted_iota(jnp.int32, (rows, rows), 0)
    row_c = lax.broadcasted_iota(jnp.int32, (rows, rows), 1)
    first = row_r - lax.rem(row_r, groups)
    lower = jnp.where((row_c >= first) & (row_c < row_r), 1.0, 0.0).astype(BF16)
    ones = jnp.ones((LANES, LANES), BF16)
    prefix = dot(stack, upper) + dot(dot(lower, stack).astype(BF16), ones)
    cat_buf[...] = jnp.zeros_like(cat_buf)
    for mb in range(n_mb):
        place = jnp.full((groups, LANES), -1.0, F32)
        for e in range(8):
            r0 = (mb * 8 + e) * groups
            slot = prefix[r0:r0 + groups]
            x_e, c_e, j = e // 4, (e // 2) % 2, e % 2
            hi = lax.rem(x_me + x_e, 2)
            g = 1 - lax.rem(y_me + j, 2) if c_e else 2 + j
            base = ((g * 2 + hi) * cap).astype(F32)
            place = jnp.where((masks[mb * 8 + e] > 0.5) & (slot < float(cap)), base + slot, place)
        slot_buf[mb] = place
        cat_buf[mb, 0:groups, :] = place
        cat_buf[mb, groups:2 * groups, :] = gate_ref[mb]
        col_buf[mb] = cat_buf[mb].T

    for c in x_loads:
        c.wait()

    def dispatch(i, _):
        g, hi, mb = piece(i)
        base = ((g * 2 + hi) * cap).astype(F32)
        want = lax.broadcasted_iota(jnp.int32, (cap, LANES), 0).astype(F32) + base
        place = slot_buf[mb]
        out = None
        for h in range(2):
            for n in range(groups // 2):
                at = h * (groups // 2) + n
                p_buf[:, n * LANES:(n + 1) * LANES] = jnp.where(place[at:at + 1, :] == want, 1.0, 0.0).astype(BF16)
            picked = dot(p_buf[...], xbuf[mb, h * (tok // 2):(h + 1) * (tok // 2), :])
            out = picked if h == 0 else (out + picked).astype(BF16)
        own = home_own(i)

        @pl.when(own)
        def _():
            recv[lax.rem(i, 8), part(c_me), :] = out

        @pl.when(jnp.logical_not(own))
        def _():
            send[send_at(i)] = out

        @pl.when((i > 0) & jnp.logical_not(home_own(i - 1)))
        def _():
            tok_copy(i - 1).start()

        return 0

    lax.fori_loop(0, 16, dispatch, 0)

    @pl.when(is_b)
    def _():
        tok_copy(15).start()

    def wait_tokens(b, _):
        for sub in range(2):
            @pl.when(jnp.logical_not(slot_own(b, sub)))
            def _():
                tok_arrival(b, sub).wait_recv()
        return 0

    def wait_weights(k):
        for local, remote in zip(w_local(0, k), w_remote(0, k)):
            local.wait()
            remote.wait()

    def pre(rows_in, k):
        return dot(rows_in, wg_buf[k]), dot(rows_in, wu_buf[k])

    def hidden(gate_up):
        gate_pre, up_pre = gate_up
        return (gate_pre / (1.0 + jnp.exp(-gate_pre)) * up_pre).astype(BF16)

    def post(gate_up, k):
        return dot(hidden(gate_up), wd_buf[k])

    def clear(b, _):
        oacc[b] = jnp.zeros_like(oacc[b])
        return 0

    def add_chunk(k, lo, hi):
        def pair(p, _):
            one = jnp.where(is_a, p * 2, jnp.where(p < 2, p * 6, p))
            two = jnp.where(is_a | (p < 2), one + 1, p + 2)
            both = [(b, pre(recv[b], k)) for b in (one, two)]
            for b, pre_b in both:
                oacc[b] += post(pre_b, k)
            return 0

        lax.fori_loop(lo, hi, pair, 0)

    def slot_of(r):
        t = lax.div(r, 2)
        straight = 2 + lax.rem(t, 2) * 2 + lax.div(t, 2)
        return jnp.where(is_a | (t >= 6), t, jnp.where(t < 4, straight, t - 4)), lax.rem(r, 2)

    def finish(start, lo, hi, chunks, ready=False):
        def one(r, _):
            b_old, sub_old = slot_of(r - 1)

            @pl.when((r > start) & jnp.logical_not(slot_own(b_old, sub_old)))
            def _():
                ret_do(b_old, sub_old, lambda c: c.start())

            b, sub = slot_of(r)
            rows_in = recv[b, part(sub), :]
            total = oacc[b, part(sub), :]
            if ready:
                total = total + dot(h_buf[part(sub), :], wd_buf[nf - 1])
            for k in chunks:
                total = total + post(pre(rows_in, k), k)
            res = total.astype(BF16)
            own = slot_own(b, sub)

            @pl.when(own)
            def _():
                back[(1 - c_me) * 2 + lax.div(b, 4), lax.rem(b, 2), 0:cap, :] = res

            @pl.when(jnp.logical_not(own))
            def _():
                recv[b, part(sub), :] = res

            return 0

        lax.fori_loop(lo, hi, one, 0)

    def combine(g, mb, width=2 * cap):
        for hi in range(width // cap):
            i = g * 4 + (1 - hi) * 2 + mb

            @pl.when(jnp.logical_not(home_own(i)))
            def _():
                ret_arrival(i).wait_recv()

        want = lax.broadcasted_iota(jnp.int32, (LANES, width), 1).astype(F32) + (g * 2 * cap).astype(F32)
        size = c_buf.shape[0]
        for blk in range(tok // size):
            for s in range(size // LANES):
                n = blk * (size // LANES) + s
                c_buf[s * LANES:(s + 1) * LANES, 0:width] = jnp.where(col_buf[mb, :, n:n + 1] == want, 1.0, 0.0).astype(BF16)
            picked = dot(c_buf[:, 0:width], back[g, mb, 0:width, :])
            for s in range(size // LANES):
                n = blk * (size // LANES) + s
                at = slice(n * LANES, (n + 1) * LANES)
                gate = col_buf[mb, :, groups + n:groups + n + 1]
                xbuf[mb, at, :] = (xbuf[mb, at, :].astype(F32) + gate * picked[s * LANES:(s + 1) * LANES, :]).astype(BF16)

    @pl.when(is_a)
    def _():
        pl.semaphore_wait(go, 1)
        lax.fori_loop(0, nf, start_remote, 0)

        def expert(j, _):
            lo, hi = j * 4, j * 4 + 4
            lax.fori_loop(lo, hi, clear, 0)
            lax.fori_loop(lo, hi, wait_tokens, 0)

            def refill(k):
                @pl.when(j == 0)
                def _():
                    pl.semaphore_signal(credit, inc=1, device_id=y_other)
                    pl.semaphore_wait(credit, 1)
                    for c in w_remote(1, k) + w_local(1, k):
                        c.start()

            def chunk(k, _):
                wait_weights(k)
                add_chunk(k, j * 2, j * 2 + 2)
                refill(k)

                return 0

            lax.fori_loop(0, nf - 1, chunk, 0)
            last_parts = list(zip(w_local(0, nf - 1), w_remote(0, nf - 1)))
            for n, (local, remote) in enumerate(last_parts):
                local.wait()
                remote.wait()
                if n == SIGNAL_AFTER:
                    @pl.when(j == 1)
                    def _():
                        pl.semaphore_signal(go, inc=1, device_id=device(0, 0, 1))

            finish(lo * 2, lo * 2, hi * 2, (nf - 1,))
            ret_copy(hi - 1, 1).start()
            refill(nf - 1)
            return 0

        lax.fori_loop(0, 2, expert, 0)

    def combine_both(g):
        def step(mb, _):
            combine(g, mb)
            return 0

        lax.fori_loop(0, n_mb, step, 0)

    @pl.when(is_b)
    def _():
        for c in w_remote(j_out, early - 3):
            c.wait_send()
        pl.semaphore_signal(go, inc=1, device_id=device(0, 0, 0))
        lax.fori_loop(0, 8, clear, 0)
        lax.fori_loop(0, 8, wait_tokens, 0)

        def chunk(k, _):
            for c in w_local(0, k):
                c.wait()
            for c in w_remote(0, k):
                c.wait_recv()

            @pl.when(k != early - 3)
            def _():
                for c in w_remote(0, k):
                    c.wait_send()

            add_chunk(k, jnp.where(k == nf - 2, 1, 0), jnp.where(k == nf - 2, 3, 4))

            @pl.when(k == early - 1)
            def _():
                combine_both(jnp.int32(2))
                pl.semaphore_wait(go, 1)
                lax.fori_loop(early, nf, start_remote, 0)

            return 0

        lax.fori_loop(0, nf - 1, chunk, 0)
        for n, (local, remote) in enumerate(zip(w_local(0, nf - 1), w_remote(0, nf - 1))):
            local.wait()
            remote.wait()
            if n == 1:
                h_buf[...] = hidden(pre(recv[2], nf - 1))
        finish(0, 0, 2, (), ready=True)
        finish(0, 2, 4, (nf - 1,))
        finish(0, 4, 12, (nf - 2, nf - 1))
        finish(0, 12, 16, (nf - 1,))

    def late(n, _):
        pair = lax.div(n, 2)
        g = jnp.where(pair < 2, pair + 2, 3 - pair)
        combine(g, lax.rem(n, 2))
        return 0

    lax.fori_loop(2 * c_me, 6, late, 0)
    outs = [pltpu.make_async_copy(xbuf.at[mb], y_hbm.at[mb], y_sem.at[mb]) for mb in range(n_mb)]
    col_out = pltpu.make_async_copy(col_buf.at[1], col_hbm, col_sem)
    combine(jnp.int32(0), jnp.int32(1), cap)
    outs[1].start()
    col_out.start()
    combine(jnp.int32(0), jnp.int32(0))
    outs[0].start()
    pltpu.make_async_remote_copy(send.at[0], tail_hbm, ret_send.at[0], ret_recv.at[1],
                                 device_id=device(1, 0, 0)).wait_recv()

    def drain(i, _):
        @pl.when(jnp.logical_not(home_own(i)))
        def _():
            tok_copy(i).wait_send()

        b, sub = lax.div(i, 2), lax.rem(i, 2)

        @pl.when(jnp.logical_not(slot_own(b, sub)))
        def _():
            ret_do(b, sub, lambda c: c.wait_send())

        return 0

    lax.fori_loop(0, 16, drain, 0)
    for c in outs + [col_out]:
        c.wait()


def tail_kernel(cap, y_hbm, col_hbm, tail_hbm, out_hbm, buf, col, tail, c_buf, in_sem, out_sem, col_sem, tail_sem):
    n_mb, tok, _ = buf.shape
    parts = 4
    size = tok // parts
    per = size // LANES
    groups = tok // LANES
    loads = [pltpu.make_async_copy(col_hbm, col, col_sem), pltpu.make_async_copy(tail_hbm, tail, tail_sem)]
    for c in loads:
        c.start()

    def rows_at(p):
        return p // parts, pl.ds((p % parts) * size, size)

    def move(p, out):
        mb, at = rows_at(p)
        if out:
            return pltpu.make_async_copy(buf.at[mb, at, :], out_hbm.at[mb, at, :], out_sem.at[p])
        return pltpu.make_async_copy(y_hbm.at[mb, at, :], buf.at[mb, at, :], in_sem.at[p])

    for p in range(n_mb * parts):
        move(p, False).start()
    loads[0].wait()
    want = lax.broadcasted_iota(jnp.int32, (LANES, cap), 1).astype(F32) + float(cap)
    for n in range(groups):
        c_buf[n * LANES:(n + 1) * LANES, :] = jnp.where(col[:, n:n + 1] == want, 1.0, 0.0).astype(BF16)
    loads[1].wait()
    for p in range(parts):
        move(p, False).wait()
        move(p, True).start()
    for p in range(parts, 2 * parts):
        blk = p - parts
        picked = dot(c_buf[blk * size:(blk + 1) * size, :], tail[...])
        move(p, False).wait()
        for s in range(per):
            n = blk * per + s
            at = slice(n * LANES, (n + 1) * LANES)
            gate = col[:, groups + n:groups + n + 1]
            part = picked[s * LANES:(s + 1) * LANES, :]
            buf[1, at, :] = (buf[1, at, :].astype(F32) + gate * part).astype(BF16)
        move(p, True).start()
    for p in range(2 * parts):
        move(p, True).wait()


def solution(mesh):
    row_spec = P(None, ('rep', 'expert', 'data'), None)
    up_spec = P('expert', 'data', None)
    down_spec = P('expert', None, 'data')

    def per_device(x_loc, idx_loc, gate_loc, wg_loc, wu_loc, wd_loc):
        n_mb, tok, d_model = x_loc.shape
        n_loc, half, ff = wg_loc.shape
        n_exp = n_loc * mesh.shape['expert']
        n_top = idx_loc.shape[2]
        assert n_top == 1 and n_exp == 8 and n_mb == 2
        cap = 8 * ((5 * n_top * tok + 32 * n_exp - 1) // (32 * n_exp))
        fc = 256
        nf = ff // fc
        early = 8
        groups = tok // LANES
        hbm = pl.BlockSpec(memory_space=pl.ANY)
        dma = pltpu.SemaphoreType.DMA
        y_part, col, tail = pl.pallas_call(
            functools.partial(moe_kernel, (cap, fc, nf, early)),
            out_shape=(jax.ShapeDtypeStruct(x_loc.shape, BF16), jax.ShapeDtypeStruct((LANES, LANES), F32),
                       jax.ShapeDtypeStruct((cap, d_model), BF16)),
            in_specs=[hbm] * 6,
            out_specs=(hbm, hbm, hbm),
            scratch_shapes=[
                pltpu.VMEM((n_mb, groups, LANES), jnp.int32), pltpu.VMEM((n_mb, groups, LANES), F32),
                pltpu.VMEM((2 * cap, fc), BF16),
                pltpu.VMEM((n_mb, tok, d_model), BF16),
                pltpu.VMEM((14, cap, d_model), BF16),
                pltpu.VMEM((8, 2 * cap, d_model), BF16),
                pltpu.VMEM((4, n_mb, 2 * cap, d_model), BF16),
                pltpu.VMEM((8, 2 * cap, d_model), F32),
                pltpu.VMEM((nf, d_model, fc), BF16),
                pltpu.VMEM((nf, d_model, fc), BF16),
                pltpu.VMEM((nf, fc, d_model), BF16),
                pltpu.VMEM((cap, tok // 2), BF16),
                pltpu.VMEM((512, 2 * cap), BF16),
                pltpu.VMEM((n_mb, groups, LANES), F32),
                pltpu.VMEM((n_mb, LANES, LANES), F32),
                pltpu.VMEM((n_mb, LANES, LANES), F32),
                dma((2,)), dma((n_mb,)), dma((n_mb,)), dma,
                dma((16,)), dma((16,)), dma((16,)), dma((16,)),
                dma((nf, 3)), dma((nf, 3)), dma((nf, 3)),
                pltpu.SemaphoreType.REGULAR, pltpu.SemaphoreType.REGULAR,
            ],
            compiler_params=pltpu.CompilerParams(
                collective_id=0, has_side_effects=True, vmem_limit_bytes=64 * 1024 * 1024 - 65536),
        )(idx_loc.reshape(n_mb, groups, LANES), gate_loc.reshape(n_mb, groups, LANES), x_loc, wg_loc, wu_loc, wd_loc)
        return pl.pallas_call(
            functools.partial(tail_kernel, cap),
            out_shape=jax.ShapeDtypeStruct(x_loc.shape, BF16),
            in_specs=[hbm, hbm, hbm],
            out_specs=hbm,
            scratch_shapes=[
                pltpu.VMEM((n_mb, tok, d_model), BF16), pltpu.VMEM((LANES, LANES), F32), pltpu.VMEM((cap, d_model), BF16),
                pltpu.VMEM((tok, cap), BF16), dma((8,)), dma((8,)), dma, dma,
            ],
        )(y_part, col, tail)

    return jax.shard_map(per_device, mesh=mesh, in_specs=(row_spec, row_spec, row_spec, up_spec, up_spec, down_spec),
                         out_specs=row_spec, check_vma=False)
```
